32 devices in a mesh: grp: 2 (over x), patch: 16 (over z, y, core).
Axes of the slice: x: 2, y: 2, z: 4, core: 2. Of those that a mesh axis runs over, the one named last changes fastest.
Arguments:
- features: bfloat16 [4, 16, 32, 640], P('grp', 'patch'), parts along dimension 0, may hold values from -6 to 6
- stale_conv_in: bfloat16 [4, 16, 32, 640], P('grp', 'patch'), parts along dimension 0, may hold values from -4.1875 to 4.1875
- stale_normed: bfloat16 [4, 16, 32, 640], P('grp', 'patch'), parts along dimension 0, may hold values from -6 to 6
- first_gain: float32 [640], replicated, may hold values from 0.1 to 1.9
- first_bias: float32 [640], replicated, may hold values from -1.8 to 1.8
- conv_weight: bfloat16 [3, 3, 640, 640], replicated, may hold values from -0.078125 to 0.078125
- conv_bias: float32 [640], replicated, may hold values from -1.8 to 1.8
- second_gain: float32 [640], replicated, may hold values from 0.1 to 1.9
- second_bias: float32 [640], replicated, may hold values from -1.8 to 1.8
- query_weight: bfloat16 [640, 640], replicated, may hold values from -6 to 6
- key_weight: bfloat16 [640, 640], replicated, may hold values from -6 to 6
- value_weight: bfloat16 [640, 640], replicated, may hold values from -0.25 to 0.25
- output_weight: bfloat16 [640, 640], replicated, may hold values from -0.25 to 0.25
- layer_gain: float32 [640], replicated, may hold values from 0.1 to 1.9
- cross_query: bfloat16 [640, 640], replicated, may hold values from -0.5 to 0.5
- cross_output: bfloat16 [640, 640], replicated, may hold values from -0.25 to 0.25
- text_keys: bfloat16 [4, 77, 640], P('grp'), parts along dimension 0, may hold values from -32 to 32
- text_values: bfloat16 [4, 77, 640], P('grp'), parts along dimension 0, may hold values from -6 to 6
Outputs:
- block_output: float32 [4, 16, 32, 640], P('grp', 'patch'), parts along dimension 0
The draws below stay inside these ranges and needn't reach their ends.
There are 2 independent parts, one for each index of `grp`. The reference program is written for one: setup_inputs(seed, part) draws one part's arguments, and reference() takes and returns one part's arrays. A program takes and returns all parts, laid end to end along the dimension named above; an argument that names none is the same for every part. Nothing has to cross between parts.
All inputs are finite; a program needn't handle non-finite values.
Results may differ from the reference program's by a relative error of at most 0.02.
The reference program's roundings to bfloat16 on the way count: a program that leaves them out, or rounds other values in their place, can miss the bound.
Values may be sent and summed in bfloat16 or wider, within the bound.
A program may use at most 128 MiB of HBM per device.

```python
import jax
import jax.numpy as jnp
from jax import lax

C = 640
GROUPS = 32
HEADS = 10
HEAD_DIM = 64
CTX = 77
HALF = 32
ATT = 640
IMAGES = 2
PATCHES = 16


def draw_features(key, part):
    key_noise = jax.random.fold_in(key, 11)
    key_channel = jax.random.fold_in(key, 12)
    place = jnp.arange(PATCHES, dtype=jnp.float32) / (PATCHES - 1)
    row_scale = (0.6 + 1.2 * place)[None, :, None, None]
    channel_scale = jax.random.uniform(key_channel, (1, 1, 1, C), jnp.float32, 0.5, 1.5)
    noise = jax.random.normal(key_noise, (IMAGES, PATCHES, HALF, C), jnp.float32)
    values = noise * row_scale * channel_scale
    return jnp.clip(values, -6.0, 6.0).astype(jnp.bfloat16)


def drawn_weight(key, salt, spread):
    key_noise = jax.random.fold_in(key, salt)
    values = jax.random.normal(key_noise, (C, ATT), jnp.float32) * spread
    return jnp.clip(values, -6.0, 6.0).astype(jnp.bfloat16)


def draw_query_weight(key, part):
    return drawn_weight(key, 81, (C // 9) ** (-0.5))


def draw_key_weight(key, part):
    return drawn_weight(key, 82, C ** (-0.5))


def draw_text_keys(key, part):
    key_noise = jax.random.fold_in(key, 91)
    values = jnp.clip(jax.random.normal(key_noise, (IMAGES, CTX, ATT), jnp.float32), -6.0, 6.0)
    return jnp.clip(values, -32.0, 32.0).astype(jnp.bfloat16)


def levels(own_key, shape, cuts, smallest, high):
    gain, own = 1.0, jax.random.fold_in(own_key, 6)
    for axis_at, blocks in cuts:
        draws = jnp.exp(jax.random.uniform(jax.random.fold_in(own, axis_at), (blocks,), jnp.float32, smallest / len(cuts), high / len(cuts)))
        gain = gain * jnp.repeat(draws, shape[axis_at] // blocks).reshape([-1 if axis == axis_at else 1 for axis in range(len(shape))])
    return gain


def gaussian(own_key, dims, scale, reach, shards=(), kind=jnp.bfloat16):
    factor_of = levels(own_key, dims, shards, -0.22, 0.18) if shards else 1.0
    array = jax.random.normal(own_key, dims, jnp.float32) * scale * factor_of
    return jnp.minimum(jnp.maximum(array, -reach), reach).astype(kind)


def setup_inputs(seed: int = 0, part: int = 0) -> dict:
    splits = jax.random.split(jax.random.key(seed), 19)
    part_keys = jax.random.split(jax.random.fold_in(splits[18], part), 19)
    return {
        "features": draw_features(jax.random.fold_in(jax.random.fold_in(splits[18], part), 71), part),
        "stale_conv_in": gaussian(part_keys[1], (IMAGES, PATCHES, HALF, C), 0.7, 4.1875, ((1, 16),)),
        "stale_normed": gaussian(part_keys[2], (IMAGES, PATCHES, HALF, C), 1.0, 6.0, ((1, 16),)),
        "first_gain": jnp.clip(1.0 + 0.18 * jax.random.normal(splits[3], (C,), jnp.float32), 0.1, 1.9),
        "first_bias": gaussian(splits[4], (C,), 0.3, 1.8, (), jnp.float32),
        "conv_weight": gaussian(splits[5], (3, 3, C, C), (9 * C) ** -0.5, 0.078125),
        "conv_bias": gaussian(splits[6], (C,), 0.3, 1.8, (), jnp.float32),
        "second_gain": jnp.clip(1.0 + 0.18 * jax.random.normal(splits[7], (C,), jnp.float32), 0.1, 1.9),
        "second_bias": gaussian(splits[8], (C,), 0.3, 1.8, (), jnp.float32),
        "query_weight": draw_query_weight(jax.random.fold_in(splits[18], 71), part),
        "key_weight": draw_key_weight(jax.random.fold_in(splits[18], 71), part),
        "value_weight": gaussian(splits[11], (C, ATT), C ** -0.5, 0.25),
        "output_weight": gaussian(splits[12], (ATT, C), ATT ** -0.5, 0.25),
        "layer_gain": jnp.clip(1.0 + 0.18 * jax.random.normal(splits[13], (C,), jnp.float32), 0.1, 1.9),
        "cross_query": gaussian(splits[14], (C, ATT), (C // 4) ** -0.5, 0.5),
        "cross_output": gaussian(splits[15], (ATT, C), ATT ** -0.5, 0.25),
        "text_keys": draw_text_keys(jax.random.fold_in(jax.random.fold_in(splits[18], part), 71), part),
        "text_values": gaussian(part_keys[17], (IMAGES, CTX, ATT), 1.0, 6.0),
    }


EPSILON = 1e-05

def narrow_exact(values):
    return lax.optimization_barrier(values.astype(jnp.bfloat16)).astype(jnp.float32)

def project(values, weight):
    return jnp.dot(values, weight, preferred_element_type=jnp.float32).astype(jnp.bfloat16)

def group_norm(features, scale_vec, shift_vec):
    images, patches, columns, channels = features.shape
    grouped = features.astype(jnp.float32).reshape(images, patches, columns, GROUPS, channels // GROUPS)
    group_mean = lax.optimization_barrier(jnp.mean(grouped, axis=(1, 2, 4), keepdims=True))
    group_var = lax.optimization_barrier(jnp.mean(jnp.square(grouped - group_mean), axis=(1, 2, 4), keepdims=True))
    normed = ((grouped - group_mean) * lax.rsqrt(group_var + EPSILON)).reshape(features.shape)
    return normed * scale_vec + shift_vec

def layer_norm(values, scale_vec):
    layer_mean = lax.optimization_barrier(jnp.mean(values, axis=-1, keepdims=True))
    centred = values - layer_mean
    layer_var = lax.optimization_barrier(jnp.mean(centred * centred, axis=-1, keepdims=True))
    return centred * lax.rsqrt(layer_var + EPSILON) * scale_vec

def patch_conv(fresh, stale, conv_weight):
    images = fresh.shape[0]
    row_count = PATCHES // 2
    image = stale.reshape(images, row_count, 2 * HALF, C)
    padded = jnp.pad(image, ((0, 0), (1, 1), (1, 1), (0, 0)))
    halves = []
    for half_side in range(2):
        columns_cut = padded[:, :, half_side * HALF:half_side * HALF + HALF + 2]
        halves.append(jnp.stack([columns_cut[:, offset:offset + row_count] for offset in range(3)], axis=2))
    windows = jnp.stack(halves, axis=2)
    centre = fresh.reshape(images, row_count, 2, HALF, C)
    windows = windows.at[:, :, :, 1, 1:HALF + 1].set(centre)
    total = jnp.zeros((images * row_count * 2 * HALF, C), jnp.float32)
    for offset_row in range(3):
        for offset_col in range(3):
            tap = windows[:, :, :, offset_row, offset_col:offset_col + HALF].reshape(-1, C)
            total = total + jnp.dot(tap, conv_weight[offset_row, offset_col], preferred_element_type=jnp.float32)
    return total.reshape(images, PATCHES, HALF, C)

def softmax_apply(queries, keys, values, scale):
    scores = jnp.einsum('bqhd,bkhd->bhqk', queries.astype(jnp.float32), keys.astype(jnp.float32)) * scale
    maxima = lax.optimization_barrier(jnp.max(scores, axis=-1, keepdims=True))
    weights = jnp.exp(scores - maxima)
    totals = lax.optimization_barrier(jnp.sum(weights, axis=-1))
    numer = jnp.einsum('bhqk,bkhd->bhqd', narrow_exact(weights), values.astype(jnp.float32))
    return numer / totals[..., None]

def reference(features, stale_conv_in, stale_normed, first_gain, first_bias, conv_weight, conv_bias, second_gain, second_bias, query_weight, key_weight, value_weight, output_weight, layer_gain, cross_query, cross_output, text_keys, text_values):
    images = features.shape[0]
    scale = HEAD_DIM ** (-0.5)
    conv_input = jax.nn.silu(group_norm(features, first_gain, first_bias)).astype(jnp.bfloat16)
    conv_out = patch_conv(conv_input, stale_conv_in, conv_weight)
    hidden = features.astype(jnp.float32) + conv_out + conv_bias
    attn_input = group_norm(hidden, second_gain, second_bias).astype(jnp.bfloat16)
    flat_input = attn_input.reshape(-1, C)
    stale_flat = stale_normed.reshape(-1, C)
    shape_att = (images, PATCHES, HALF, ATT)
    queries = project(flat_input, query_weight).reshape(shape_att)
    fresh_keys = project(flat_input, key_weight).reshape(shape_att)
    fresh_values = project(flat_input, value_weight).reshape(shape_att)
    stale_keys = project(stale_flat, key_weight).reshape(shape_att)
    stale_values = project(stale_flat, value_weight).reshape(shape_att)

    def one_patch(position):
        patch_queries = lax.dynamic_slice_in_dim(queries, position, 1, 1).reshape(images, HALF, HEADS, HEAD_DIM)
        own_keys = lax.dynamic_slice_in_dim(fresh_keys, position, 1, 1)
        own_values = lax.dynamic_slice_in_dim(fresh_values, position, 1, 1)
        keys_all = lax.dynamic_update_slice_in_dim(stale_keys, own_keys, position, 1).reshape(images, PATCHES * HALF, HEADS, HEAD_DIM)
        values_all = lax.dynamic_update_slice_in_dim(stale_values, own_values, position, 1).reshape(images, PATCHES * HALF, HEADS, HEAD_DIM)
        result = softmax_apply(patch_queries, keys_all, values_all, scale)
        return result.transpose(0, 2, 1, 3).reshape(images, HALF, ATT).astype(jnp.bfloat16)
    attended = lax.map(one_patch, jnp.arange(PATCHES, dtype=jnp.int32)).transpose(1, 0, 2, 3)
    mixed = hidden.reshape(-1, C) + jnp.dot(attended.reshape(-1, ATT), output_weight, preferred_element_type=jnp.float32)
    layer_in = layer_norm(mixed, layer_gain).astype(jnp.bfloat16)
    cross_q = project(layer_in, cross_query).reshape(images, PATCHES * HALF, HEADS, HEAD_DIM)
    text_k = text_keys.reshape(images, CTX, HEADS, HEAD_DIM)
    text_v = text_values.reshape(images, CTX, HEADS, HEAD_DIM)
    cross_result = softmax_apply(cross_q, text_k, text_v, scale)
    cross_attn = cross_result.transpose(0, 2, 1, 3).reshape(-1, ATT).astype(jnp.bfloat16)
    block_output = mixed + jnp.dot(cross_attn, cross_output, preferred_element_type=jnp.float32)
    return block_output.reshape(images, PATCHES, HALF, C)
```

```python
import functools

import jax
import jax.numpy as jnp
from jax import lax
from jax.experimental import pallas as pl
from jax.experimental.pallas import tpu as pltpu
from jax.sharding import PartitionSpec as P

GROUPS = 32
HEADS = 10
HEAD_DIM = 64
EPSILON = 1e-05
MESH = pl.DeviceIdType.MESH
LANES = 128
F32 = jnp.float32
BF16 = jnp.bfloat16


def mark(name):
    pass


def dot(a, b, **kw):
    return jnp.dot(a, b, preferred_element_type=F32, **kw)


def dot_t(a, b):
    return lax.dot_general(a, b, (((1,), (1,)), ((), ())), preferred_element_type=F32)


def group_matrix(channels, transposed):
    width = channels // GROUPS
    shape = (LANES, channels) if transposed else (channels, LANES)
    channel = lax.broadcasted_iota(jnp.int32, shape, 1 if transposed else 0)
    group = lax.broadcasted_iota(jnp.int32, shape, 0 if transposed else 1)
    inside = (channel >= group * width) & (channel < (group + 1) * width)
    return jnp.where(inside, 1.0, 0.0).astype(BF16)


def split_dot(x, selector):
    high = x.astype(BF16)
    rest = x - high.astype(F32)
    middle = rest.astype(BF16)
    low = (rest - middle.astype(F32)).astype(BF16)
    made = dot(jnp.concatenate([high, middle, low], axis=0), selector)
    n = x.shape[0]
    return made[:n] + made[n:2 * n] + made[2 * n:]


def attention_stages(units, lane):
    low = lane < HEAD_DIM
    scores = []
    for q, k, _ in units:
        both = jnp.concatenate([jnp.where(low, q, 0.0), jnp.where(low, 0.0, q)], axis=0)
        scores.append(dot_t(both.astype(BF16), k))
    weights = [jnp.exp(s - jnp.max(s, axis=-1, keepdims=True)) for s in scores]
    totals = [jnp.sum(w, axis=-1, keepdims=True) for w in weights]
    outs = [dot(w.astype(BF16), v) for w, (_, _, v) in zip(weights, units)]
    outs = [o / t for o, t in zip(outs, totals)]
    cols = lane.shape[0]
    return [jnp.where(low, o[:cols], o[cols:]) for o in outs]


def kernel(
    patches, images, cols,
    feat_h, sconv_h, snorm_h, fg_h, fb_h, wc_h, cb_h, sg_h, sb_h,
    wq_h, wk_h, wv_h, wo_h, lg_h, wcq_h, wco_h, tk_h, tv_h,
    out_ref,
    feat, sconv, xall, kv, wc, ws, v0, v1, v2, v3, v4, v5, tk_in, tv_in, tk, tv,
    stats, halo, edge_src, edges, lhs, taps, att,
    st_send, st_recv, xz_send, relay_send, xy_send, x_recv, kv_send, kv_recv,
    halo_send, halo_recv, edge_send, edge_recv, in_sem, wc_sem, w_sem, v_sem,
):
    channels = feat.shape[-1]
    rows = images * cols
    outer = patches // 4
    chips = patches // 2
    me = lax.axis_index("patch")
    chip, core = me // 2, me % 2
    zo, yi = chip // 2, chip % 2
    other = 1 - yi
    partner = chip * 2 + (1 - core)

    def index(o, i, c):
        return (o * 2 + i) * 2 + c

    def at_slot(slot):
        return pl.ds(pl.multiple_of(slot * cols, cols), cols)

    cp_feat = pltpu.make_async_copy(feat_h, feat, in_sem.at[0])
    cp_sconv = pltpu.make_async_copy(sconv_h, sconv, in_sem.at[1])
    cp_snorm = pltpu.make_async_copy(snorm_h, xall.at[:, at_slot(me), :], in_sem.at[2])
    cp_tk = pltpu.make_async_copy(tk_h, tk_in, in_sem.at[3])
    cp_tv = pltpu.make_async_copy(tv_h, tv_in, in_sem.at[4])
    cp_feat.start()
    cp_sconv.start()
    cp_snorm.start()
    cp_vec = [
        pltpu.make_async_copy(h, own_vec, v_sem.at[t])
        for t, (h, own_vec) in enumerate(zip((fg_h, fb_h, cb_h, sg_h, sb_h, lg_h), (v0, v1, v2, v3, v4, v5)))
    ]
    for c in cp_vec:
        c.start()
    barrier = pltpu.get_barrier_semaphore()

    def greet(d, carry):
        pl.semaphore_signal(
            barrier, inc=1, device_id={"patch": lax.rem(me + d, patches)}, device_id_type=MESH
        )
        return carry

    row_first, row_last = chip == 0, chip == chips - 1

    @pl.when(row_first)
    def _():
        halo[0] = jnp.zeros(halo.shape[1:], BF16)
        edges[0] = jnp.zeros(edges.shape[1:], F32)

    @pl.when(row_last)
    def _():
        halo[1] = jnp.zeros(halo.shape[1:], BF16)
        edges[2] = jnp.zeros(edges.shape[1:], F32)

    lax.fori_loop(1, patches, greet, 0)
    cp_wc = {}
    for i in (2, 1, 0):
        cp_wc[i] = pltpu.make_async_copy(wc_h.at[i], wc.at[i], wc_sem.at[i])
        cp_wc[i].start()
    cp_w = [
        pltpu.make_async_copy(h, ws.at[t], w_sem.at[t])
        for t, h in enumerate((wk_h, wv_h, wq_h, wo_h, wcq_h, wco_h))
    ]
    for c in cp_w:
        c.start()
    cp_tk.start()
    cp_tv.start()

    gather_groups = group_matrix(channels, False)
    spread_groups = group_matrix(channels, True)
    count = float(patches * cols * (channels // GROUPS))

    def local_stats(phase, x):
        sums = [jnp.sum(x[b * cols:(b + 1) * cols], axis=0, keepdims=True) for b in range(images)]
        squares = [
            jnp.sum(x[b * cols:(b + 1) * cols] * x[b * cols:(b + 1) * cols], axis=0, keepdims=True)
            for b in range(images)
        ]
        table = jnp.concatenate(sums + squares, axis=0)
        stats[phase, me] = split_dot(table, gather_groups)

    def stat_copy(phase, ref, target):
        return pltpu.make_async_remote_copy(
            src_ref=ref, dst_ref=ref, send_sem=st_send.at[phase], recv_sem=st_recv.at[phase],
            device_id={"patch": target}, device_id_type=MESH,
        )

    def send_stats(phase):
        def body(d, carry):
            stat_copy(phase, stats.at[phase, me], lax.rem(me + d, patches)).start()
            return carry
        lax.fori_loop(1, patches, body, 0)

    def all_stats(phase):
        return stat_copy(phase, stats.at[phase, pl.ds(0, patches - 1)], partner)

    def finish_stats(phase):
        all_stats(phase).wait_recv()
        total = jnp.sum(stats[phase], axis=0) / count
        mean = total[:images]
        var = total[images:] - mean * mean
        table = jnp.concatenate([mean, lax.rsqrt(var + EPSILON)], axis=0)
        return split_dot(table, spread_groups)

    def normed(x, table, b, gain, bias):
        part = x[b * cols:(b + 1) * cols]
        return (part - table[b:b + 1]) * table[images + b:images + b + 1] * gain + bias

    def x_copy(b, z, y, target, send):
        ref = xall.at[b, at_slot(index(z, y, core)), :]
        return pltpu.make_async_remote_copy(
            src_ref=ref, dst_ref=ref, send_sem=send, recv_sem=x_recv.at[b, z * 2 + y],
            device_id={"patch": target}, device_id_type=MESH,
        )

    def kv_copy(ref, which):
        return pltpu.make_async_remote_copy(
            src_ref=ref, dst_ref=ref, send_sem=kv_send.at[which], recv_sem=kv_recv,
            device_id={"patch": partner}, device_id_type=MESH,
        )

    def halo_copy(which, step):
        return pltpu.make_async_remote_copy(
            src_ref=sconv, dst_ref=halo.at[which], send_sem=halo_send.at[which],
            recv_sem=halo_recv.at[which],
            device_id={"patch": lax.rem(me + 2 * step + patches, patches)}, device_id_type=MESH,
        )

    def edge_copy(which, step):
        return pltpu.make_async_remote_copy(
            src_ref=edge_src, dst_ref=edges.at[which], send_sem=edge_send.at[which],
            recv_sem=edge_recv.at[which],
            device_id={"patch": lax.rem(partner + 2 * step + patches, patches)}, device_id_type=MESH,
        )

    mark("stats0")
    cp_feat.wait()
    x = feat[...].reshape(rows, channels).astype(F32)
    local_stats(0, x)
    mark("edges")
    cp_sconv.wait()
    whole_conv = sconv[...].astype(F32)
    edge_src[...] = jnp.where(core == 0, whole_conv[:, cols - 1], whole_conv[:, 0])
    for c in cp_vec:
        c.wait()
    vec = [v[...].reshape(1, channels) for v in (v0, v1, v2, v3, v4, v5)]
    cp_snorm.wait()

    def near(distance, visit):
        @pl.when(zo + distance < outer)
        def _():
            visit(zo + distance, 0)

        @pl.when(zo - distance >= 0)
        def _():
            visit(zo - distance, 1)

    def send_own(distance):
        def visit(z, way):
            for b in range(images):
                x_copy(b, zo, yi, index(z, yi, core), xz_send.at[distance - 1, way]).start()
        near(distance, visit)

    mark("barrier")
    pl.semaphore_wait(barrier, patches - 1)
    mark("sends")
    send_stats(0)
    edge_copy(1, 0).start()

    @pl.when(jnp.logical_not(row_last))
    def _():
        halo_copy(0, 1).start()
        edge_copy(0, 1).start()

    @pl.when(jnp.logical_not(row_first))
    def _():
        halo_copy(1, -1).start()
        edge_copy(2, -1).start()

    for b in range(images):
        x_copy(b, zo, yi, index(zo, other, core), xy_send).start()
    send_own(1)
    mark("text")
    cp_tk.wait()
    cp_tv.wait()
    for b in range(images):
        tk[b] = tk_in[:, b, :]
        tv[b] = tv_in[:, b, :]
    if outer > 2:
        send_own(2)

    def pass_z(z, way):
        distance = jnp.abs(z - zo)
        onward = zo - 1 + 2 * way
        go_on = (distance >= 2) & (onward >= 0) & (onward < outer)
        for b in range(images):
            x_copy(b, z, yi, partner, xy_send).wait_recv()
            x_copy(b, z, yi, index(zo, other, core), xy_send).start()

            @pl.when(go_on)
            def _():
                x_copy(b, z, yi, index(onward, yi, core), relay_send.at[z]).start()

    def stale_kv(z):
        for b in range(images):
            x_copy(b, z, other, partner, xy_send).wait_recv()
        places = [(b, at_slot(index(z, y, core))) for b in range(images) for y in range(2)]
        block = jnp.concatenate([xall[b, at, :] for b, at in places], axis=0)
        for w in range(2):
            made = dot(block, ws[w]).astype(BF16)
            for t, (b, at) in enumerate(places):
                kv[w, b, at, :] = made[t * cols:(t + 1) * cols]

    def push_kv(z):
        for y in range(2):
            at = at_slot(index(z, y, core))
            ref = kv.at[:, :, at, :]

            @pl.when((z == zo) & (yi == y))
            def _():
                kv_copy(ref, 0).start()

            @pl.when((z != zo) | (yi != y))
            def _():
                kv_copy(ref, 1).start()

    def row_taps(i):
        cp_wc[i].wait()
        for j in range(3):
            made = dot(lhs[i], wc[i, j])
            taps[j] = made if i == 2 else taps[j] + made

    def fill_row(i, cells):
        for b in range(images):
            lhs[i, b * cols:(b + 1) * cols, :] = cells[b]
        filler = jnp.zeros((lhs.shape[1] - rows - images, channels), F32)
        lhs[i, rows:, :] = jnp.concatenate([edges[i], filler], axis=0).astype(BF16)

    mark("halo1")

    @pl.when(jnp.logical_not(row_last))
    def _():
        halo_copy(1, -1).wait_recv()
        edge_copy(2, -1).wait_recv()

    mark("conv2")
    fill_row(2, halo[1])
    row_taps(2)
    mark("wait0")
    table = finish_stats(0)
    mark("norm0")
    edge_copy(1, 0).wait_recv()
    centre = []
    for b in range(images):
        v = normed(x, table, b, vec[0], vec[1])
        centre.append((v * (1.0 / (1.0 + jnp.exp(-v)))).astype(BF16))
    fill_row(1, centre)
    mark("conv1")
    row_taps(1)
    mark("halo0")

    @pl.when(jnp.logical_not(row_first))
    def _():
        halo_copy(0, 1).wait_recv()
        edge_copy(0, 1).wait_recv()

    mark("conv0")
    fill_row(0, halo[0])
    row_taps(0)
    mark("shift")
    place = lax.broadcasted_iota(jnp.int32, (cols, channels), 0)
    parts = []
    for b in range(images):
        at = slice(b * cols, (b + 1) * cols)
        left = pltpu.roll(taps[0, at], 1, 0)
        right = pltpu.roll(taps[2, at], cols - 1, 0)
        left_edge = jnp.where(core == 1, taps[0, rows + b:rows + b + 1], 0.0)
        right_edge = jnp.where(core == 0, taps[2, rows + b:rows + b + 1], 0.0)
        left = jnp.where(place == 0, left_edge, left)
        right = jnp.where(place == cols - 1, right_edge, right)
        conv = left + taps[1, at] + right
        parts.append(x[at] + conv + vec[2])
    hidden = jnp.concatenate(parts, axis=0)
    mark("stats1")
    local_stats(1, hidden)
    mark("send1")
    send_stats(1)
    mark("pass1")
    near(1, pass_z)
    mark("kv0")
    cp_w[0].wait()
    cp_w[1].wait()
    stale_kv(zo)
    push_kv(zo)

    def step(distance, carry):
        @pl.when(distance + 1 < outer)
        def _():
            near(distance + 1, pass_z)

        def visit(z, way):
            stale_kv(z)
            push_kv(z)

        near(distance, visit)
        return carry

    mark("kvs")
    lax.fori_loop(1, outer, step, 0)
    mark("wait1")
    cp_w[2].wait()
    table = finish_stats(1)
    mark("norm1")
    attn_in = jnp.concatenate(
        [normed(hidden, table, b, vec[3], vec[4]) for b in range(images)], axis=0
    ).astype(BF16)
    own = at_slot(me)
    kv_copy(kv.at[:, :, own, :], 0).wait_send()
    for w in range(2):
        fresh = dot(attn_in, ws[w]).astype(BF16)
        for b in range(images):
            kv[w, b, own, :] = fresh[b * cols:(b + 1) * cols]
    mark("q")
    scale = HEAD_DIM ** -0.5
    lane = lax.broadcasted_iota(jnp.int32, (cols, LANES), 1)
    pairs = channels // LANES

    def heads(q, keys, values, together):
        for first in range(0, images, together):
            places = [
                (b, slice(p * LANES, (p + 1) * LANES))
                for b in range(first, first + together) for p in range(pairs)
            ]
            units = [
                (q[b * cols:(b + 1) * cols, at], keys[b, :, at], values[b, :, at])
                for b, at in places
            ]
            for (b, at), part in zip(places, attention_stages(units, lane)):
                att[b * cols:(b + 1) * cols, at] = part.astype(BF16)

    query = dot(attn_in, ws[2]).astype(BF16).astype(F32) * scale
    mark("kvwait")
    kv_copy(kv.at[0], 1).wait_recv()
    mark("attend")
    heads(query, kv.at[0], kv.at[1], 1)
    mark("out_ln")
    cp_w[3].wait()
    mixed = hidden + dot(att[...], ws[3])
    centred = mixed - jnp.mean(mixed, axis=-1, keepdims=True)
    variance = jnp.mean(centred * centred, axis=-1, keepdims=True)
    layer_in = (centred * lax.rsqrt(variance + EPSILON) * vec[5]).astype(BF16)
    mark("cross")
    cp_w[4].wait()
    heads(dot(layer_in, ws[4]).astype(BF16).astype(F32) * scale, tk, tv, images)
    mark("out")
    cp_w[5].wait()
    out_ref[...] = mixed + dot(att[...], ws[5])

    mark("drain")
    all_stats(0).wait_send()
    all_stats(1).wait_send()
    pltpu.make_async_remote_copy(
        src_ref=xall.at[0, pl.ds(0, outer * images * cols)], dst_ref=xall.at[0, pl.ds(0, outer * images * cols)],
        send_sem=xy_send, recv_sem=x_recv.at[0, 0],
        device_id={"patch": partner}, device_id_type=MESH,
    ).wait_send()
    kv_copy(kv.at[0, :, pl.ds(0, (patches - 2) * cols)], 1).wait_send()

    def drain_z(distance):
        def visit(z, way):
            pltpu.make_async_remote_copy(
                src_ref=xall.at[:, at_slot(me), :], dst_ref=xall.at[:, at_slot(me), :],
                send_sem=xz_send.at[distance - 1, way], recv_sem=x_recv.at[0, 0],
                device_id={"patch": partner}, device_id_type=MESH,
            ).wait_send()
        near(distance, visit)

    drain_z(1)
    if outer > 2:
        drain_z(2)

    def drain_relay(z, carry):
        onward = jnp.where(z < zo, zo + 1, zo - 1)

        @pl.when((jnp.abs(z - zo) >= 2) & (onward >= 0) & (onward < outer))
        def _():
            pltpu.make_async_remote_copy(
                src_ref=xall.at[:, at_slot(me), :], dst_ref=xall.at[:, at_slot(me), :],
                send_sem=relay_send.at[z], recv_sem=x_recv.at[0, 0],
                device_id={"patch": partner}, device_id_type=MESH,
            ).wait_send()
        return carry

    if outer > 3:
        lax.fori_loop(0, outer, drain_relay, 0)
    edge_copy(1, 0).wait_send()

    @pl.when(jnp.logical_not(row_last))
    def _():
        halo_copy(0, 1).wait_send()
        edge_copy(0, 1).wait_send()

    @pl.when(jnp.logical_not(row_first))
    def _():
        halo_copy(1, -1).wait_send()
        edge_copy(2, -1).wait_send()


def solution(mesh):
    patches = mesh.shape["patch"]

    def on_device(
        features, stale_conv_in, stale_normed, first_gain, first_bias, conv_weight, conv_bias,
        second_gain, second_bias, query_weight, key_weight, value_weight, output_weight,
        layer_gain, cross_query, cross_output, text_keys, text_values,
    ):
        images, _, cols, channels = features.shape
        rows = images * cols
        span = patches * cols
        outer = patches // 4
        ctx = text_keys.shape[1]

        def flat(a):
            return a.reshape(images, cols, channels)

        dma = pltpu.SemaphoreType.DMA
        out = pl.pallas_call(
            functools.partial(kernel, patches, images, cols),
            out_shape=pltpu.VMEM((rows, channels), F32),
            in_specs=[pl.BlockSpec(memory_space=pltpu.HBM)] * 18,
            out_specs=pl.BlockSpec(memory_space=pltpu.VMEM),
            scratch_shapes=[
                pltpu.VMEM((images, cols, channels), BF16),
                pltpu.VMEM((images, cols, channels), BF16),
                pltpu.VMEM((images, span, channels), BF16),
                pltpu.VMEM((2, images, span, channels), BF16),
                pltpu.VMEM(conv_weight.shape, BF16),
                pltpu.VMEM((6, channels, channels), BF16),
                *[pltpu.VMEM((channels,), F32)] * 6,
                pltpu.VMEM((ctx, images, channels), BF16),
                pltpu.VMEM((ctx, images, channels), BF16),
                pltpu.VMEM((images, ctx, channels), BF16),
                pltpu.VMEM((images, ctx, channels), BF16),
                pltpu.VMEM((2, patches, 2 * images, LANES), F32),
                pltpu.VMEM((2, images, cols, channels), BF16),
                pltpu.VMEM((images, channels), F32),
                pltpu.VMEM((3, images, channels), F32),
                pltpu.VMEM((3, rows + 16, channels), BF16),
                pltpu.VMEM((3, rows + 16, channels), F32),
                pltpu.VMEM((rows, channels), BF16),
                dma((2,)), dma((2,)), dma((2, 2)), dma((outer,)), dma,
                dma((images, 2 * outer)), dma((2,)), dma,
                dma((2,)), dma((2,)), dma((3,)), dma((3,)),
                dma((5,)), dma((3,)), dma((6,)), dma((6,)),
            ],
            compiler_params=pltpu.CompilerParams(
                collective_id=0, has_side_effects=True, vmem_limit_bytes=60000 * 1024
            ),
        )(
            flat(features), flat(stale_conv_in), flat(stale_normed), first_gain, first_bias,
            conv_weight, conv_bias, second_gain, second_bias, query_weight, key_weight,
            value_weight, output_weight, layer_gain, cross_query, cross_output,
            text_keys.transpose(1, 0, 2), text_values.transpose(1, 0, 2),
        )
        return out.reshape(features.shape)

    act = P("grp", "patch", None, None)
    text = P("grp", None, None)
    return jax.shard_map(
        on_device, mesh=mesh,
        in_specs=(act,) * 3 + (P(),) * 13 + (text,) * 2,
        out_specs=act, check_vma=False,
    )
```

```python
import functools

import jax
import jax.numpy as jnp
from jax import lax
from jax.experimental import pallas as pl
from jax.experimental.pallas import tpu as pltpu
from jax.sharding import PartitionSpec as P

GROUPS = 32
HEADS = 10
HEAD_DIM = 64
EPSILON = 1e-05
MESH = pl.DeviceIdType.MESH
LANES = 128
F32 = jnp.float32
BF16 = jnp.bfloat16


def mark(name):
    pass


def dot(a, b, **kw):
    return jnp.dot(a, b, preferred_element_type=F32, **kw)


def dot_t(a, b):
    return lax.dot_general(a, b, (((1,), (1,)), ((), ())), preferred_element_type=F32)


def group_matrix(channels, transposed):
    width = channels // GROUPS
    shape = (LANES, channels) if transposed else (channels, LANES)
    channel = lax.broadcasted_iota(jnp.int32, shape, 1 if transposed else 0)
    group = lax.broadcasted_iota(jnp.int32, shape, 0 if transposed else 1)
    inside = (channel >= group * width) & (channel < (group + 1) * width)
    return jnp.where(inside, 1.0, 0.0).astype(BF16)


def split_dot(x, selector):
    high = x.astype(BF16)
    rest = x - high.astype(F32)
    middle = rest.astype(BF16)
    low = (rest - middle.astype(F32)).astype(BF16)
    made = dot(jnp.concatenate([high, middle, low], axis=0), selector)
    n = x.shape[0]
    return made[:n] + made[n:2 * n] + made[2 * n:]


def attention_stages(units, lane):
    low = lane < HEAD_DIM
    scores = []
    for q, k, _ in units:
        both = jnp.concatenate([jnp.where(low, q, 0.0), jnp.where(low, 0.0, q)], axis=0)
        scores.append(dot_t(both.astype(BF16), k))
    weights = [jnp.exp(s - jnp.max(s, axis=-1, keepdims=True)) for s in scores]
    totals = [jnp.sum(w, axis=-1, keepdims=True) for w in weights]
    outs = [dot(w.astype(BF16), v) for w, (_, _, v) in zip(weights, units)]
    outs = [o / t for o, t in zip(outs, totals)]
    cols = lane.shape[0]
    return [jnp.where(low, o[:cols], o[cols:]) for o in outs]


def kernel(
    patches, images, cols,
    feat_h, sconv_h, snorm_h, fg_h, fb_h, wc_h, cb_h, sg_h, sb_h,
    wq_h, wk_h, wv_h, wo_h, lg_h, wcq_h, wco_h, tk_h, tv_h,
    out_ref,
    feat, sconv, xall, kv, wc, ws, v0, v1, v2, v3, v4, v5, tk_in, tv_in, tk, tv,
    stats, halo, edge_src, edges, lhs, taps, att,
    st_send, st_recv, xz_send, xy_send, x_recv, kv_send, kv_recv,
    halo_send, halo_recv, edge_send, edge_recv, ready, in_sem, wc_sem, w_sem, v_sem,
):
    channels = feat.shape[-1]
    rows = images * cols
    outer = patches // 4
    chips = patches // 2
    me = lax.axis_index("patch")
    chip, core = me // 2, me % 2
    zo, yi = chip // 2, chip % 2
    other = 1 - yi
    first = jnp.where(zo > 0, zo - 1, 1)
    partner = chip * 2 + (1 - core)

    def index(o, i, c):
        return (o * 2 + i) * 2 + c

    def at_slot(slot):
        return pl.ds(pl.multiple_of(slot * cols, cols), cols)

    cp_feat = pltpu.make_async_copy(feat_h, feat, in_sem.at[0])
    cp_sconv = pltpu.make_async_copy(sconv_h, sconv, in_sem.at[1])
    cp_snorm = pltpu.make_async_copy(snorm_h, xall.at[:, at_slot(me), :], in_sem.at[2])
    cp_tk = pltpu.make_async_copy(tk_h, tk_in, in_sem.at[3])
    cp_tv = pltpu.make_async_copy(tv_h, tv_in, in_sem.at[4])
    cp_feat.start()
    cp_sconv.start()
    cp_snorm.start()
    cp_vec = [
        pltpu.make_async_copy(h, own_vec, v_sem.at[t])
        for t, (h, own_vec) in enumerate(zip((fg_h, fb_h, cb_h, sg_h, sb_h, lg_h), (v0, v1, v2, v3, v4, v5)))
    ]
    for c in cp_vec:
        c.start()
    barrier = pltpu.get_barrier_semaphore()

    hub = outer - 1
    early = zo < hub
    expected = jnp.where(early, 4 * zo + 5 + 2 * yi, patches - 1)

    def greet(d, carry):
        target = lax.rem(me + d, patches)
        tz, ty = target // 4, (target // 2) % 2
        next_up = (zo == tz + 1) & ((yi == ty) | (chip == target // 2 + 1))

        @pl.when((tz >= hub) | (zo <= tz) | next_up)
        def _():
            pl.semaphore_signal(
                barrier, inc=1, device_id={"patch": target}, device_id_type=MESH
            )
        return carry

    row_first, row_last = chip == 0, chip == chips - 1

    @pl.when(row_first)
    def _():
        halo[0] = jnp.zeros(halo.shape[1:], BF16)
        edges[0] = jnp.zeros(edges.shape[1:], F32)

    @pl.when(row_last)
    def _():
        halo[1] = jnp.zeros(halo.shape[1:], BF16)
        edges[2] = jnp.zeros(edges.shape[1:], F32)

    lax.fori_loop(1, patches, greet, 0)
    cp_wc = {}
    for i in (2, 0, 1):
        cp_wc[i] = pltpu.make_async_copy(wc_h.at[i], wc.at[i], wc_sem.at[i])
        cp_wc[i].start()
    cp_w = [
        pltpu.make_async_copy(h, ws.at[t], w_sem.at[t])
        for t, h in enumerate((wk_h, wv_h, wq_h, wo_h, wcq_h, wco_h))
    ]
    for c in cp_w:
        c.start()
    cp_tk.start()
    cp_tv.start()

    gather_groups = group_matrix(channels, False)
    spread_groups = group_matrix(channels, True)
    count = float(patches * cols * (channels // GROUPS))

    def local_stats(phase, x):
        sums = [jnp.sum(x[b * cols:(b + 1) * cols], axis=0, keepdims=True) for b in range(images)]
        squares = [
            jnp.sum(x[b * cols:(b + 1) * cols] * x[b * cols:(b + 1) * cols], axis=0, keepdims=True)
            for b in range(images)
        ]
        table = jnp.concatenate(sums + squares, axis=0)
        stats[phase, me] = split_dot(table, gather_groups)

    def stat_copy(phase, ref, target):
        return pltpu.make_async_remote_copy(
            src_ref=ref, dst_ref=ref, send_sem=st_send.at[phase], recv_sem=st_recv.at[phase],
            device_id={"patch": target}, device_id_type=MESH,
        )

    def send_stats(phase, wanted=None):
        def body(d, carry):
            target = lax.rem(me + d, patches)

            def send():
                stat_copy(phase, stats.at[phase, me], target).start()

            if wanted is None:
                send()
            else:
                pl.when(wanted(target // 4))(send)
            return carry
        lax.fori_loop(1, patches, body, 0)

    def all_stats(phase):
        return stat_copy(phase, stats.at[phase, pl.ds(0, patches - 1)], partner)

    def finish_stats(phase):
        all_stats(phase).wait_recv()
        total = jnp.sum(stats[phase], axis=0) / count
        mean = total[:images]
        var = total[images:] - mean * mean
        table = jnp.concatenate([mean, lax.rsqrt(var + EPSILON)], axis=0)
        return split_dot(table, spread_groups)

    def normed(x, table, b, gain, bias):
        part = x[b * cols:(b + 1) * cols]
        return (part - table[b:b + 1]) * table[images + b:images + b + 1] * gain + bias

    def x_copy(b, z, y, target, send):
        ref = xall.at[b, at_slot(index(z, y, core)), :]
        return pltpu.make_async_remote_copy(
            src_ref=ref, dst_ref=ref, send_sem=send, recv_sem=x_recv.at[b, z * 2 + y],
            device_id={"patch": target}, device_id_type=MESH,
        )

    def kv_copy(ref, which):
        return pltpu.make_async_remote_copy(
            src_ref=ref, dst_ref=ref, send_sem=kv_send.at[which], recv_sem=kv_recv,
            device_id={"patch": partner}, device_id_type=MESH,
        )

    def halo_copy(which, step):
        return pltpu.make_async_remote_copy(
            src_ref=sconv, dst_ref=halo.at[which], send_sem=halo_send.at[which],
            recv_sem=halo_recv.at[which],
            device_id={"patch": lax.rem(me + 2 * step + patches, patches)}, device_id_type=MESH,
        )

    def edge_copy(which, step):
        return pltpu.make_async_remote_copy(
            src_ref=edge_src, dst_ref=edges.at[which], send_sem=edge_send.at[which],
            recv_sem=edge_recv.at[which],
            device_id={"patch": lax.rem(partner + 2 * step + patches, patches)}, device_id_type=MESH,
        )

    mark("stats0")
    cp_feat.wait()
    x = feat[...].reshape(rows, channels).astype(F32)
    local_stats(0, x)
    mark("edges")
    cp_sconv.wait()
    whole_conv = sconv[...].astype(F32)
    edge_src[...] = jnp.where(core == 0, whole_conv[:, cols - 1], whole_conv[:, 0])
    for c in cp_vec:
        c.wait()
    vec = [v[...].reshape(1, channels) for v in (v0, v1, v2, v3, v4, v5)]
    cp_snorm.wait()

    def near(distance, visit):
        @pl.when(zo + distance < outer)
        def _():
            visit(zo + distance, 0)

        @pl.when(zo - distance >= 0)
        def _():
            visit(zo - distance, 1)

    def send_to(z):
        for b in range(images):
            x_copy(b, zo, yi, index(z, yi, core), xz_send).start()

    def send_far(first, last):
        def body(step, carry):
            near(last - step, lambda z, way: send_known(z))
            return carry

        def send_known(z):
            @pl.when(((zo >= hub) | (z < zo + 2)) & ((zo != 1) | (z != 0)))
            def _():
                send_to(z)

        lax.fori_loop(0, last - first + 1, body, 0)

    mark("barrier")
    pl.semaphore_wait(barrier, expected)
    mark("sends")

    def tell(z, carry):
        pl.semaphore_signal(
            ready, inc=1, device_id={"patch": index(z, yi, core)}, device_id_type=MESH
        )
        return carry

    @pl.when(zo == hub)
    def _():
        lax.fori_loop(0, hub, tell, 0)

    send_stats(0, lambda z: (zo >= hub) | (z <= zo))
    edge_copy(1, 0).start()

    @pl.when(yi == 0)
    def _():
        edge_copy(0, 1).start()
        halo_copy(0, 1).start()

    @pl.when(yi == 1)
    def _():
        edge_copy(2, -1).start()
        halo_copy(1, -1).start()

    for b in range(images):
        x_copy(b, zo, yi, index(zo, other, core), xy_send).start()
    if outer > 3:
        send_far(3, outer - 1)

    @pl.when(zo == 1)
    def _():
        send_to(0)

    @pl.when((yi == 0) & jnp.logical_not(row_first))
    def _():
        edge_copy(2, -1).start()
        halo_copy(1, -1).start()

    send_far(1, min(2, outer - 1))
    mark("ready")

    @pl.when(early)
    def _():
        pl.semaphore_wait(ready, 1)
        send_stats(0, lambda z: z > zo)

        @pl.when(yi == 1)
        def _():
            edge_copy(0, 1).start()
            halo_copy(0, 1).start()

        def late(step, carry):
            send_to(outer - 1 - step)
            return carry

        lax.fori_loop(0, outer - 2 - zo, late, 0)

    def wait_x(b, z, y):
        x_copy(b, z, y, partner, xy_send).wait_recv()

    def pass_y(z):
        for b in range(images):
            wait_x(b, z, yi)
            x_copy(b, z, yi, index(zo, other, core), xy_send).start()

    def distance_at(step):
        return jnp.where(zo < outer // 2, outer - step, step)

    def each_far(visit):
        def body(step, carry):
            def one(z, way):
                @pl.when(z != first)
                def _():
                    visit(z)
            near(distance_at(step), one)
            return carry
        return body

    def stale_kv(z):
        places = [(b, at_slot(index(z, y, core))) for b in range(images) for y in range(2)]
        block = jnp.concatenate([xall[b, at, :] for b, at in places], axis=0)
        for w in range(2):
            made = dot(block, ws[w]).astype(BF16)
            for t, (b, at) in enumerate(places):
                kv[w, b, at, :] = made[t * cols:(t + 1) * cols]

    def push_kv(z):
        for y in range(2):
            at = at_slot(index(z, y, core))
            ref = kv.at[:, :, at, :]

            @pl.when((z == zo) & (yi == y))
            def _():
                kv_copy(ref, 0).start()

            @pl.when((z != zo) | (yi != y))
            def _():
                kv_copy(ref, 1).start()

    def row_taps(i, first=False):
        for j in range(3):
            made = dot(lhs[i], wc[i, j])
            taps[j] = made if first else taps[j] + made

    def fill_row(i, cells):
        for b in range(images):
            lhs[i, b * cols:(b + 1) * cols, :] = cells[b]
        filler = jnp.zeros((lhs.shape[1] - rows - images, channels), F32)
        lhs[i, rows:, :] = jnp.concatenate([edges[i], filler], axis=0).astype(BF16)

    mark("pass0")
    pass_y(first)

    def outside(beside):
        mark("halo%d" % beside)
        below = (yi == 0) if beside else (yi == 1)
        which = jnp.where(below, 1, 0)
        row = 2 * which

        @pl.when(below & jnp.logical_not(row_last))
        def _():
            halo_copy(1, -1).wait_recv()
            edge_copy(2, -1).wait_recv()

        @pl.when(jnp.logical_not(below) & jnp.logical_not(row_first))
        def _():
            halo_copy(0, 1).wait_recv()
            edge_copy(0, 1).wait_recv()

        mark("conv%d" % beside)
        fill_row(row, halo[which])
        row_taps(row, beside)

    for i in range(3):
        cp_wc[i].wait()
    outside(True)
    mark("wait0")
    table = finish_stats(0)
    mark("norm0")
    edge_copy(1, 0).wait_recv()
    centre = []
    for b in range(images):
        v = normed(x, table, b, vec[0], vec[1])
        centre.append((v * (1.0 / (1.0 + jnp.exp(-v)))).astype(BF16))
    fill_row(1, centre)
    mark("conv1")
    row_taps(1)
    outside(False)
    mark("shift")
    place = lax.broadcasted_iota(jnp.int32, (cols, channels), 0)
    parts = []
    for b in range(images):
        at = slice(b * cols, (b + 1) * cols)
        left = pltpu.roll(taps[0, at], 1, 0)
        right = pltpu.roll(taps[2, at], cols - 1, 0)
        left_edge = jnp.where(core == 1, taps[0, rows + b:rows + b + 1], 0.0)
        right_edge = jnp.where(core == 0, taps[2, rows + b:rows + b + 1], 0.0)
        left = jnp.where(place == 0, left_edge, left)
        right = jnp.where(place == cols - 1, right_edge, right)
        conv = left + taps[1, at] + right
        parts.append(x[at] + conv + vec[2])
    hidden = jnp.concatenate(parts, axis=0)
    mark("stats1")
    local_stats(1, hidden)
    mark("send1")
    send_stats(1)
    mark("pass1")
    pass_far = each_far(pass_y)
    lax.fori_loop(1, min(2, outer), pass_far, 0)
    mark("kv_own")
    cp_w[0].wait()
    cp_w[1].wait()
    for b in range(images):
        wait_x(b, zo, other)
    stale_kv(zo)
    push_kv(zo)
    mark("pass2")
    lax.fori_loop(2, outer, pass_far, 0)
    mark("text")
    cp_tk.wait()
    cp_tv.wait()
    for b in range(images):
        tk[b] = tk_in[:, b, :]
        tv[b] = tv_in[:, b, :]

    def layer_kv(z):
        for b in range(images):
            wait_x(b, z, other)
        stale_kv(z)
        push_kv(z)

    mark("kv_first")
    layer_kv(first)

    far_kv = each_far(layer_kv)
    mark("kv_far")
    lax.fori_loop(1, outer - 1, far_kv, 0)
    mark("wait1")
    cp_w[2].wait()
    table = finish_stats(1)
    mark("norm1")
    attn_in = jnp.concatenate(
        [normed(hidden, table, b, vec[3], vec[4]) for b in range(images)], axis=0
    ).astype(BF16)
    own = at_slot(me)
    kv_copy(kv.at[:, :, own, :], 0).wait_send()
    for w in range(2):
        fresh = dot(attn_in, ws[w]).astype(BF16)
        for b in range(images):
            kv[w, b, own, :] = fresh[b * cols:(b + 1) * cols]
    mark("q")
    scale = HEAD_DIM ** -0.5
    lane = lax.broadcasted_iota(jnp.int32, (cols, LANES), 1)
    pairs = channels // LANES

    def heads(q, keys, values, together):
        for first in range(0, images, together):
            places = [
                (b, slice(p * LANES, (p + 1) * LANES))
                for b in range(first, first + together) for p in range(pairs)
            ]
            units = [
                (q[b * cols:(b + 1) * cols, at], keys[b, :, at], values[b, :, at])
                for b, at in places
            ]
            for (b, at), part in zip(places, attention_stages(units, lane)):
                att[b * cols:(b + 1) * cols, at] = part.astype(BF16)

    query = dot(attn_in, ws[2]).astype(BF16).astype(F32) * scale
    mark("kv_last")
    lax.fori_loop(outer - 1, outer, far_kv, 0)
    mark("kvwait")
    kv_copy(kv.at[0], 1).wait_recv()
    mark("attend")
    heads(query, kv.at[0], kv.at[1], 1)
    mark("out_ln")
    cp_w[3].wait()
    mixed = hidden + dot(att[...], ws[3])
    centred = mixed - jnp.mean(mixed, axis=-1, keepdims=True)
    variance = jnp.mean(centred * centred, axis=-1, keepdims=True)
    layer_in = (centred * lax.rsqrt(variance + EPSILON) * vec[5]).astype(BF16)
    mark("cross")
    cp_w[4].wait()
    heads(dot(layer_in, ws[4]).astype(BF16).astype(F32) * scale, tk, tv, images)
    mark("out")
    cp_w[5].wait()
    out_ref[...] = mixed + dot(att[...], ws[5])

    mark("drain")
    all_stats(0).wait_send()
    all_stats(1).wait_send()
    def sent(blocks, send):
        for b in range(images):
            ref = xall.at[b, pl.ds(0, blocks * cols), :]
            pltpu.make_async_remote_copy(
                src_ref=ref, dst_ref=ref, send_sem=send, recv_sem=x_recv.at[0, 0],
                device_id={"patch": partner}, device_id_type=MESH,
            ).wait_send()

    sent(outer - 1, xz_send)

    sent(outer, xy_send)
    kv_copy(kv.at[0, :, pl.ds(0, (patches - 2) * cols)], 1).wait_send()
    edge_copy(1, 0).wait_send()

    @pl.when(jnp.logical_not(row_last))
    def _():
        halo_copy(0, 1).wait_send()
        edge_copy(0, 1).wait_send()

    @pl.when(jnp.logical_not(row_first))
    def _():
        halo_copy(1, -1).wait_send()
        edge_copy(2, -1).wait_send()


def solution(mesh):
    patches = mesh.shape["patch"]

    def on_device(
        features, stale_conv_in, stale_normed, first_gain, first_bias, conv_weight, conv_bias,
        second_gain, second_bias, query_weight, key_weight, value_weight, output_weight,
        layer_gain, cross_query, cross_output, text_keys, text_values,
    ):
        images, _, cols, channels = features.shape
        rows = images * cols
        span = patches * cols
        outer = patches // 4
        ctx = text_keys.shape[1]

        def flat(a):
            return a.reshape(images, cols, channels)

        dma = pltpu.SemaphoreType.DMA
        out = pl.pallas_call(
            functools.partial(kernel, patches, images, cols),
            out_shape=pltpu.VMEM((rows, channels), F32),
            in_specs=[pl.BlockSpec(memory_space=pltpu.HBM)] * 18,
            out_specs=pl.BlockSpec(memory_space=pltpu.VMEM),
            scratch_shapes=[
                pltpu.VMEM((images, cols, channels), BF16),
                pltpu.VMEM((images, cols, channels), BF16),
                pltpu.VMEM((images, span, channels), BF16),
                pltpu.VMEM((2, images, span, channels), BF16),
                pltpu.VMEM(conv_weight.shape, BF16),
                pltpu.VMEM((6, channels, channels), BF16),
                *[pltpu.VMEM((channels,), F32)] * 6,
                pltpu.VMEM((ctx, images, channels), BF16),
                pltpu.VMEM((ctx, images, channels), BF16),
                pltpu.VMEM((images, ctx, channels), BF16),
                pltpu.VMEM((images, ctx, channels), BF16),
                pltpu.VMEM((2, patches, 2 * images, LANES), F32),
                pltpu.VMEM((2, images, cols, channels), BF16),
                pltpu.VMEM((images, channels), F32),
                pltpu.VMEM((3, images, channels), F32),
                pltpu.VMEM((3, rows + 16, channels), BF16),
                pltpu.VMEM((3, rows + 16, channels), F32),
                pltpu.VMEM((rows, channels), BF16),
                dma((2,)), dma((2,)), dma, dma,
                dma((images, 2 * outer)), dma((2,)), dma,
                dma((2,)), dma((2,)), dma((3,)), dma((3,)), pltpu.SemaphoreType.REGULAR,
                dma((5,)), dma((3,)), dma((6,)), dma((6,)),
            ],
            compiler_params=pltpu.CompilerParams(
                collective_id=0, has_side_effects=True, vmem_limit_bytes=60000 * 1024
            ),
        )(
            flat(features), flat(stale_conv_in), flat(stale_normed), first_gain, first_bias,
            conv_weight, conv_bias, second_gain, second_bias, query_weight, key_weight,
            value_weight, output_weight, layer_gain, cross_query, cross_output,
            text_keys.transpose(1, 0, 2), text_values.transpose(1, 0, 2),
        )
        return out.reshape(features.shape)

    act = P("grp", "patch", None, None)
    text = P("grp", None, None)
    return jax.shard_map(
        on_device, mesh=mesh,
        in_specs=(act,) * 3 + (P(),) * 13 + (text,) * 2,
        out_specs=act, check_vma=False,
    )
```

```python
import functools

import jax
import jax.numpy as jnp
from jax import lax
from jax.experimental import pallas as pl
from jax.experimental.pallas import tpu as pltpu
from jax.sharding import PartitionSpec as P

GROUPS = 32
HEADS = 10
HEAD_DIM = 64
EPSILON = 1e-05
MESH = pl.DeviceIdType.MESH
LANES = 128
F32 = jnp.float32
BF16 = jnp.bfloat16


def mark(name):
    pass


def dot(a, b, **kw):
    return jnp.dot(a, b, preferred_element_type=F32, **kw)


def dot_t(a, b):
    return lax.dot_general(a, b, (((1,), (1,)), ((), ())), preferred_element_type=F32)


def group_matrix(channels, transposed):
    width = channels // GROUPS
    shape = (LANES, channels) if transposed else (channels, LANES)
    channel = lax.broadcasted_iota(jnp.int32, shape, 1 if transposed else 0)
    group = lax.broadcasted_iota(jnp.int32, shape, 0 if transposed else 1)
    inside = (channel >= group * width) & (channel < (group + 1) * width)
    return jnp.where(inside, 1.0, 0.0).astype(BF16)


def split_dot(x, selector):
    high = x.astype(BF16)
    rest = x - high.astype(F32)
    middle = rest.astype(BF16)
    low = (rest - middle.astype(F32)).astype(BF16)
    made = dot(jnp.concatenate([high, middle, low], axis=0), selector)
    n = x.shape[0]
    return made[:n] + made[n:2 * n] + made[2 * n:]


def attention_stages(units, lane):
    low = lane < HEAD_DIM
    scores = []
    for q, k, _ in units:
        both = jnp.concatenate([jnp.where(low, q, 0.0), jnp.where(low, 0.0, q)], axis=0)
        scores.append(dot_t(both.astype(BF16), k))
    weights = [jnp.exp(s - jnp.max(s, axis=-1, keepdims=True)) for s in scores]
    totals = [jnp.sum(w, axis=-1, keepdims=True) for w in weights]
    outs = [dot(w.astype(BF16), v) for w, (_, _, v) in zip(weights, units)]
    outs = [o / t for o, t in zip(outs, totals)]
    cols = lane.shape[0]
    return [jnp.where(low, o[:cols], o[cols:]) for o in outs]


def kernel(
    patches, images, cols,
    feat_h, sconv_h, snorm_h, fg_h, fb_h, wc_h, cb_h, sg_h, sb_h,
    wq_h, wk_h, wv_h, wo_h, lg_h, wcq_h, wco_h, tk_h, tv_h,
    out_ref,
    feat, sconv, xall, kv, wc, ws, vecs, t_in, tk, tv,
    stats, halo, edge_src, edges, lhs, taps, att,
    st_send, st_recv, xz_send, xy_send, x_recv, kv_send, kv_recv,
    halo_send, halo_recv, edge_send, edge_recv, ready, in_sem, wc_sem, w_sem, v_sem,
):
    channels = feat.shape[-1]
    rows = images * cols
    outer = patches // 4
    chips = patches // 2
    me = lax.axis_index("patch")
    chip, core = me // 2, me % 2
    zo, yi = chip // 2, chip % 2
    other = 1 - yi
    first = jnp.where(zo > 0, zo - 1, 1)
    partner = chip * 2 + (1 - core)

    def index(o, i, c):
        return (o * 2 + i) * 2 + c

    def at_slot(slot):
        return pl.ds(pl.multiple_of(slot * cols, cols), cols)

    barrier = pltpu.get_barrier_semaphore()

    hub = outer - 1
    early = zo < hub
    expected = jnp.where(early, 4 * zo + 5 + 2 * yi, patches - 1)

    def greet(d, carry):
        target = lax.rem(me + d, patches)
        tz, ty = target // 4, (target // 2) % 2
        next_up = (zo == tz + 1) & ((yi == ty) | (chip == target // 2 + 1))

        @pl.when((tz >= hub) | (zo <= tz) | next_up)
        def _():
            pl.semaphore_signal(
                barrier, inc=1, device_id={"patch": target}, device_id_type=MESH
            )
        return carry

    lax.fori_loop(1, patches, greet, 0)
    cp_feat = pltpu.make_async_copy(feat_h, feat, in_sem.at[0])
    cp_sconv = pltpu.make_async_copy(sconv_h, sconv, in_sem.at[1])
    cp_snorm = pltpu.make_async_copy(snorm_h, xall.at[:, at_slot(me), :], in_sem.at[2])
    cp_text = [
        pltpu.make_async_copy(h, t_in.at[t], in_sem.at[3]) for t, h in enumerate((tk_h, tv_h))
    ]
    all_text = pltpu.make_async_copy(t_in, t_in, in_sem.at[3])
    cp_feat.start()
    cp_sconv.start()
    cp_snorm.start()
    cp_vec = [
        pltpu.make_async_copy(h, vecs.at[pl.ds(t * channels, channels)], v_sem)
        for t, h in enumerate((fg_h, fb_h, cb_h, sg_h, sb_h, lg_h))
    ]
    for c in cp_vec:
        c.start()
    row_first, row_last = chip == 0, chip == chips - 1

    @pl.when(row_first)
    def _():
        halo[0] = jnp.zeros(halo.shape[1:], BF16)
        edges[0] = jnp.zeros(edges.shape[1:], F32)

    @pl.when(row_last)
    def _():
        halo[1] = jnp.zeros(halo.shape[1:], BF16)
        edges[2] = jnp.zeros(edges.shape[1:], F32)

    for c in cp_text:
        c.start()
    cp_wc = pltpu.make_async_copy(wc_h, wc, wc_sem)
    cp_wc.start()
    cp_w = [
        pltpu.make_async_copy(h, ws.at[t], w_sem.at[t // 3])
        for t, h in enumerate((wk_h, wv_h, wq_h, wo_h, wcq_h, wco_h))
    ]

    def wait_weights(part):
        ref = ws.at[pl.ds(3 * part, 3)]
        pltpu.make_async_copy(ref, ref, w_sem.at[part]).wait()

    for c in cp_w:
        c.start()

    gather_groups = group_matrix(channels, False)
    spread_groups = group_matrix(channels, True)
    count = float(patches * cols * (channels // GROUPS))

    def local_stats(phase, x):
        sums = [jnp.sum(x[b * cols:(b + 1) * cols], axis=0, keepdims=True) for b in range(images)]
        squares = [
            jnp.sum(x[b * cols:(b + 1) * cols] * x[b * cols:(b + 1) * cols], axis=0, keepdims=True)
            for b in range(images)
        ]
        table = jnp.concatenate(sums + squares, axis=0)
        stats[phase, me] = split_dot(table, gather_groups)

    def stat_copy(phase, ref, target):
        return pltpu.make_async_remote_copy(
            src_ref=ref, dst_ref=ref, send_sem=st_send.at[phase], recv_sem=st_recv.at[phase],
            device_id={"patch": target}, device_id_type=MESH,
        )

    def send_stats(phase, wanted=None):
        def body(d, carry):
            target = lax.rem(me + d, patches)

            def send():
                stat_copy(phase, stats.at[phase, me], target).start()

            if wanted is None:
                send()
            else:
                pl.when(wanted(target // 4))(send)
            return carry
        lax.fori_loop(1, patches, body, 0)

    def all_stats(phase):
        return stat_copy(phase, stats.at[phase, pl.ds(0, patches - 1)], partner)

    def finish_stats(phase):
        all_stats(phase).wait_recv()
        total = jnp.sum(stats[phase], axis=0) / count
        mean = total[:images]
        var = total[images:] - mean * mean
        table = jnp.concatenate([mean, lax.rsqrt(var + EPSILON)], axis=0)
        return split_dot(table, spread_groups)

    def normed(x, table, b, gain, bias):
        part = x[b * cols:(b + 1) * cols]
        return (part - table[b:b + 1]) * table[images + b:images + b + 1] * gain + bias

    def x_copy(b, z, y, target, send):
        ref = xall.at[b, at_slot(index(z, y, core)), :]
        return pltpu.make_async_remote_copy(
            src_ref=ref, dst_ref=ref, send_sem=send, recv_sem=x_recv.at[b, z * 2 + y],
            device_id={"patch": target}, device_id_type=MESH,
        )

    def kv_copy(ref, which):
        return pltpu.make_async_remote_copy(
            src_ref=ref, dst_ref=ref, send_sem=kv_send.at[which], recv_sem=kv_recv,
            device_id={"patch": partner}, device_id_type=MESH,
        )

    def halo_copy(which, step):
        return pltpu.make_async_remote_copy(
            src_ref=sconv, dst_ref=halo.at[which], send_sem=halo_send.at[which],
            recv_sem=halo_recv.at[which],
            device_id={"patch": lax.rem(me + 2 * step + patches, patches)}, device_id_type=MESH,
        )

    def edge_copy(which, step):
        return pltpu.make_async_remote_copy(
            src_ref=edge_src, dst_ref=edges.at[which], send_sem=edge_send.at[which],
            recv_sem=edge_recv.at[which],
            device_id={"patch": lax.rem(partner + 2 * step + patches, patches)}, device_id_type=MESH,
        )

    mark("stats0")
    cp_feat.wait()
    x = feat[...].reshape(rows, channels).astype(F32)
    local_stats(0, x)
    mark("edges")
    cp_sconv.wait()
    whole_conv = sconv[...].astype(F32)
    edge_src[...] = jnp.where(core == 0, whole_conv[:, cols - 1], whole_conv[:, 0])
    pltpu.make_async_copy(vecs, vecs, v_sem).wait()
    vec = [vecs[pl.ds(t * channels, channels)].reshape(1, channels) for t in range(6)]
    cp_snorm.wait()

    def near(distance, visit):
        @pl.when(zo + distance < outer)
        def _():
            visit(zo + distance, 0)

        @pl.when(zo - distance >= 0)
        def _():
            visit(zo - distance, 1)

    def send_to(z):
        for b in range(images):
            x_copy(b, zo, yi, index(z, yi, core), xz_send).start()

    def send_far(first, last):
        def body(step, carry):
            near(last - step, lambda z, way: send_known(z))
            return carry

        def send_known(z):
            @pl.when(((zo >= hub) | (z < zo + 2)) & ((zo != 1) | (z != 0)))
            def _():
                send_to(z)

        lax.fori_loop(0, last - first + 1, body, 0)

    mark("barrier")
    pl.semaphore_wait(barrier, expected)
    mark("sends")

    def tell(z, carry):
        pl.semaphore_signal(
            ready, inc=1, device_id={"patch": index(z, yi, core)}, device_id_type=MESH
        )
        return carry

    @pl.when(zo == hub)
    def _():
        lax.fori_loop(0, hub, tell, 0)

    send_stats(0, lambda z: (zo >= hub) | (z <= zo))
    edge_copy(1, 0).start()

    @pl.when(yi == 0)
    def _():
        edge_copy(0, 1).start()
        halo_copy(0, 1).start()

    @pl.when(yi == 1)
    def _():
        edge_copy(2, -1).start()
        halo_copy(1, -1).start()

    for b in range(images):
        x_copy(b, zo, yi, index(zo, other, core), xy_send).start()
    if outer > 3:
        send_far(3, outer - 1)

    @pl.when(zo == 1)
    def _():
        send_to(0)

    @pl.when((yi == 0) & jnp.logical_not(row_first))
    def _():
        edge_copy(2, -1).start()
        halo_copy(1, -1).start()

    send_far(1, min(2, outer - 1))
    mark("ready")

    @pl.when(early)
    def _():
        pl.semaphore_wait(ready, 1)
        send_stats(0, lambda z: z > zo)

        @pl.when(yi == 1)
        def _():
            edge_copy(0, 1).start()
            halo_copy(0, 1).start()

        def late(step, carry):
            send_to(outer - 1 - step)
            return carry

        lax.fori_loop(0, outer - 2 - zo, late, 0)

    def wait_x(b, z, y):
        x_copy(b, z, y, partner, xy_send).wait_recv()

    def pass_y(z):
        for b in range(images):
            wait_x(b, z, yi)
            x_copy(b, z, yi, index(zo, other, core), xy_send).start()

    def distance_at(step):
        return jnp.where(zo < outer // 2, outer - step, step)

    def each_far(visit):
        def body(step, carry):
            def one(z, way):
                @pl.when(z != first)
                def _():
                    visit(z)
            near(distance_at(step), one)
            return carry
        return body

    def stale_kv(z):
        places = [(b, at_slot(index(z, y, core))) for b in range(images) for y in range(2)]
        block = jnp.concatenate([xall[b, at, :] for b, at in places], axis=0)
        for w in range(2):
            made = dot(block, ws[w]).astype(BF16)
            for t, (b, at) in enumerate(places):
                kv[w, b, at, :] = made[t * cols:(t + 1) * cols]

    def push_kv(z):
        for y in range(2):
            at = at_slot(index(z, y, core))
            ref = kv.at[:, :, at, :]

            @pl.when((z == zo) & (yi == y))
            def _():
                kv_copy(ref, 0).start()

            @pl.when((z != zo) | (yi != y))
            def _():
                kv_copy(ref, 1).start()

    def row_taps(i, first=False):
        for j in range(3):
            made = dot(lhs[i], wc[i, j])
            taps[j] = made if first else taps[j] + made

    def fill_row(i, cells):
        for b in range(images):
            lhs[i, b * cols:(b + 1) * cols, :] = cells[b]
        filler = jnp.zeros((lhs.shape[1] - rows - images, channels), F32)
        lhs[i, rows:, :] = jnp.concatenate([edges[i], filler], axis=0).astype(BF16)

    mark("pass0")
    pass_y(first)
    mark("text")
    all_text.wait()
    for b in range(images):
        tk[b] = t_in[0, :, b, :]
        tv[b] = t_in[1, :, b, :]

    def outside(beside):
        mark("halo%d" % beside)
        below = (yi == 0) if beside else (yi == 1)
        which = jnp.where(below, 1, 0)
        row = 2 * which

        @pl.when(below & jnp.logical_not(row_last))
        def _():
            halo_copy(1, -1).wait_recv()
            edge_copy(2, -1).wait_recv()

        @pl.when(jnp.logical_not(below) & jnp.logical_not(row_first))
        def _():
            halo_copy(0, 1).wait_recv()
            edge_copy(0, 1).wait_recv()

        mark("conv%d" % beside)
        fill_row(row, halo[which])
        row_taps(row, beside)

    cp_wc.wait()
    outside(True)
    pass_far = each_far(pass_y)
    mark("wait0")
    table = finish_stats(0)
    mark("norm0")
    edge_copy(1, 0).wait_recv()
    centre = []
    for b in range(images):
        v = normed(x, table, b, vec[0], vec[1])
        centre.append((v * (1.0 / (1.0 + jnp.exp(-v)))).astype(BF16))
    fill_row(1, centre)
    mark("conv1")
    row_taps(1)
    mark("pass1b")
    done = jnp.where((zo == outer - 2) & (yi == 0), outer, 2)
    done = jnp.where((zo < outer // 2) | (yi == 0) & (zo == outer - 2), done, 1)
    lax.fori_loop(1, done, pass_far, 0)
    outside(False)
    mark("shift")
    place = lax.broadcasted_iota(jnp.int32, (cols, channels), 0)
    parts = []
    for b in range(images):
        at = slice(b * cols, (b + 1) * cols)
        left = pltpu.roll(taps[0, at], 1, 0)
        right = pltpu.roll(taps[2, at], cols - 1, 0)
        left_edge = jnp.where(core == 1, taps[0, rows + b:rows + b + 1], 0.0)
        right_edge = jnp.where(core == 0, taps[2, rows + b:rows + b + 1], 0.0)
        left = jnp.where(place == 0, left_edge, left)
        right = jnp.where(place == cols - 1, right_edge, right)
        conv = left + taps[1, at] + right
        parts.append(x[at] + conv + vec[2])
    hidden = jnp.concatenate(parts, axis=0)
    mark("stats1")
    local_stats(1, hidden)
    mark("send1")
    send_stats(1)
    mark("kv_own")
    wait_weights(0)
    for b in range(images):
        wait_x(b, zo, other)
    stale_kv(zo)
    push_kv(zo)
    mark("pass2")
    lax.fori_loop(done, outer, pass_far, 0)

    def layer_kv(z):
        for b in range(images):
            wait_x(b, z, other)
        stale_kv(z)
        push_kv(z)

    mark("kv_first")
    layer_kv(first)

    far_kv = each_far(layer_kv)
    mark("kv_far")
    lax.fori_loop(1, outer, far_kv, 0)
    mark("wait1")
    table = finish_stats(1)
    mark("norm1")
    attn_in = jnp.concatenate(
        [normed(hidden, table, b, vec[3], vec[4]) for b in range(images)], axis=0
    ).astype(BF16)
    own = at_slot(me)
    kv_copy(kv.at[:, :, own, :], 0).wait_send()
    for w in range(2):
        fresh = dot(attn_in, ws[w]).astype(BF16)
        for b in range(images):
            kv[w, b, own, :] = fresh[b * cols:(b + 1) * cols]
    mark("q")
    scale = HEAD_DIM ** -0.5
    lane = lax.broadcasted_iota(jnp.int32, (cols, LANES), 1)
    pairs = channels // LANES

    def heads(q, keys, values, together):
        for first in range(0, images, together):
            places = [
                (b, slice(p * LANES, (p + 1) * LANES))
                for b in range(first, first + together) for p in range(pairs)
            ]
            units = [
                (q[b * cols:(b + 1) * cols, at], keys[b, :, at], values[b, :, at])
                for b, at in places
            ]
            for (b, at), part in zip(places, attention_stages(units, lane)):
                att[b * cols:(b + 1) * cols, at] = part.astype(BF16)

    query = dot(attn_in, ws[2]).astype(BF16).astype(F32) * scale
    mark("kvwait")
    kv_copy(kv.at[0], 1).wait_recv()
    mark("attend")
    heads(query, kv.at[0], kv.at[1], images)
    mark("out_ln")
    wait_weights(1)
    mixed = hidden + dot(att[...], ws[3])
    centred = mixed - jnp.mean(mixed, axis=-1, keepdims=True)
    variance = jnp.mean(centred * centred, axis=-1, keepdims=True)
    layer_in = (centred * lax.rsqrt(variance + EPSILON) * vec[5]).astype(BF16)
    mark("cross")
    heads(dot(layer_in, ws[4]).astype(BF16).astype(F32) * scale, tk, tv, images)
    mark("out")
    out_ref[...] = mixed + dot(att[...], ws[5])

    mark("drain")
    all_stats(0).wait_send()
    all_stats(1).wait_send()
    def sent(blocks, send):
        for b in range(images):
            ref = xall.at[b, pl.ds(0, blocks * cols), :]
            pltpu.make_async_remote_copy(
                src_ref=ref, dst_ref=ref, send_sem=send, recv_sem=x_recv.at[0, 0],
                device_id={"patch": partner}, device_id_type=MESH,
            ).wait_send()

    sent(outer - 1, xz_send)

    sent(outer, xy_send)
    kv_copy(kv.at[0, :, pl.ds(0, (patches - 2) * cols)], 1).wait_send()
    edge_copy(1, 0).wait_send()

    @pl.when(jnp.logical_not(row_last))
    def _():
        halo_copy(0, 1).wait_send()
        edge_copy(0, 1).wait_send()

    @pl.when(jnp.logical_not(row_first))
    def _():
        halo_copy(1, -1).wait_send()
        edge_copy(2, -1).wait_send()


def solution(mesh):
    patches = mesh.shape["patch"]

    def on_device(
        features, stale_conv_in, stale_normed, first_gain, first_bias, conv_weight, conv_bias,
        second_gain, second_bias, query_weight, key_weight, value_weight, output_weight,
        layer_gain, cross_query, cross_output, text_keys, text_values,
    ):
        images, _, cols, channels = features.shape
        rows = images * cols
        span = patches * cols
        outer = patches // 4
        ctx = text_keys.shape[1]

        def flat(a):
            return a.reshape(images, cols, channels)

        dma = pltpu.SemaphoreType.DMA
        out = pl.pallas_call(
            functools.partial(kernel, patches, images, cols),
            out_shape=pltpu.VMEM((rows, channels), F32),
            in_specs=[pl.BlockSpec(memory_space=pltpu.HBM)] * 18,
            out_specs=pl.BlockSpec(memory_space=pltpu.VMEM),
            scratch_shapes=[
                pltpu.VMEM((images, cols, channels), BF16),
                pltpu.VMEM((images, cols, channels), BF16),
                pltpu.VMEM((images, span, channels), BF16),
                pltpu.VMEM((2, images, span, channels), BF16),
                pltpu.VMEM(conv_weight.shape, BF16),
                pltpu.VMEM((6, channels, channels), BF16),
                pltpu.VMEM((6 * channels,), F32),
                pltpu.VMEM((2, ctx, images, channels), BF16),
                pltpu.VMEM((images, ctx, channels), BF16),
                pltpu.VMEM((images, ctx, channels), BF16),
                pltpu.VMEM((2, patches, 2 * images, LANES), F32),
                pltpu.VMEM((2, images, cols, channels), BF16),
                pltpu.VMEM((images, channels), F32),
                pltpu.VMEM((3, images, channels), F32),
                pltpu.VMEM((3, rows + 16, channels), BF16),
                pltpu.VMEM((3, rows + 16, channels), F32),
                pltpu.VMEM((rows, channels), BF16),
                dma((2,)), dma((2,)), dma, dma,
                dma((images, 2 * outer)), dma((2,)), dma,
                dma((2,)), dma((2,)), dma((3,)), dma((3,)), pltpu.SemaphoreType.REGULAR,
                dma((4,)), dma, dma((2,)), dma,
            ],
            compiler_params=pltpu.CompilerParams(
                collective_id=0, has_side_effects=True, vmem_limit_bytes=60000 * 1024
            ),
        )(
            flat(features), flat(stale_conv_in), flat(stale_normed), first_gain, first_bias,
            conv_weight, conv_bias, second_gain, second_bias, query_weight, key_weight,
            value_weight, output_weight, layer_gain, cross_query, cross_output,
            text_keys.transpose(1, 0, 2), text_values.transpose(1, 0, 2),
        )
        return out.reshape(features.shape)

    act = P("grp", "patch", None, None)
    text = P("grp", None, None)
    return jax.shard_map(
        on_device, mesh=mesh,
        in_specs=(act,) * 3 + (P(),) * 13 + (text,) * 2,
        out_specs=act, check_vma=False,
    )
```

```python
import functools

import jax
import jax.numpy as jnp
from jax import lax
from jax.experimental import pallas as pl
from jax.experimental.pallas import tpu as pltpu
from jax.sharding import PartitionSpec as P

GROUPS = 32
HEADS = 10
HEAD_DIM = 64
EPSILON = 1e-05
MESH = pl.DeviceIdType.MESH
LANES = 128
F32 = jnp.float32
BF16 = jnp.bfloat16


def mark(name):
    pass


def dot(a, b, **kw):
    return jnp.dot(a, b, preferred_element_type=F32, **kw)


def dot_t(a, b):
    return lax.dot_general(a, b, (((1,), (1,)), ((), ())), preferred_element_type=F32)


def group_matrix(channels, transposed):
    width = channels // GROUPS
    shape = (LANES, channels) if transposed else (channels, LANES)
    channel = lax.broadcasted_iota(jnp.int32, shape, 1 if transposed else 0)
    group = lax.broadcasted_iota(jnp.int32, shape, 0 if transposed else 1)
    inside = (channel >= group * width) & (channel < (group + 1) * width)
    return jnp.where(inside, 1.0, 0.0).astype(BF16)


def split_dot(x, selector):
    high = x.astype(BF16)
    rest = x - high.astype(F32)
    middle = rest.astype(BF16)
    low = (rest - middle.astype(F32)).astype(BF16)
    made = dot(jnp.concatenate([high, middle, low], axis=0), selector)
    n = x.shape[0]
    return made[:n] + made[n:2 * n] + made[2 * n:]


def attention_stages(units, lane):
    low = lane < HEAD_DIM
    scores = []
    for q, k, _ in units:
        both = jnp.concatenate([jnp.where(low, q, 0.0), jnp.where(low, 0.0, q)], axis=0)
        scores.append(dot_t(both.astype(BF16), k))
    weights = [jnp.exp(s - jnp.max(s, axis=-1, keepdims=True)) for s in scores]
    totals = [jnp.sum(w, axis=-1, keepdims=True) for w in weights]
    outs = [dot(w.astype(BF16), v) for w, (_, _, v) in zip(weights, units)]
    outs = [o / t for o, t in zip(outs, totals)]
    cols = lane.shape[0]
    return [jnp.where(low, o[:cols], o[cols:]) for o in outs]


def kernel(
    patches, images, cols,
    feat_h, sconv_h, snorm_h, fg_h, fb_h, wc_h, cb_h, sg_h, sb_h,
    wq_h, wk_h, wv_h, wo_h, lg_h, wcq_h, wco_h, tk_h, tv_h,
    out_ref,
    feat, sconv, xall, kv, wc, ws, vecs, t_in, tk, tv,
    stats, halo, edge_src, edges, lhs, taps, att,
    st_send, st_recv, xz_send, xy_send, around_send, x_recv, kv_send, kv_recv,
    halo_send, halo_recv, edge_send, edge_recv, ready, in_sem, wc_sem, w_sem, v_sem,
):
    channels = feat.shape[-1]
    rows = images * cols
    outer = patches // 4
    chips = patches // 2
    me = lax.axis_index("patch")
    chip, core = me // 2, me % 2
    zo, yi = chip // 2, chip % 2
    other = 1 - yi
    first = jnp.where(zo > 0, zo - 1, 1)
    partner = chip * 2 + (1 - core)

    def index(o, i, c):
        return (o * 2 + i) * 2 + c

    def at_slot(slot):
        return pl.ds(pl.multiple_of(slot * cols, cols), cols)

    barrier = pltpu.get_barrier_semaphore()

    hub = outer - 1
    early = zo < hub
    expected = jnp.where(early, 4 * zo + 5 + 2 * yi, patches - 1)

    def greet(d, carry):
        target = lax.rem(me + d, patches)
        tz, ty = target // 4, (target // 2) % 2
        next_up = (zo == tz + 1) & ((yi == ty) | (chip == target // 2 + 1))

        @pl.when((tz >= hub) | (zo <= tz) | next_up)
        def _():
            pl.semaphore_signal(
                barrier, inc=1, device_id={"patch": target}, device_id_type=MESH
            )
        return carry

    lax.fori_loop(1, patches, greet, 0)
    cp_feat = pltpu.make_async_copy(feat_h, feat, in_sem.at[0])
    cp_sconv = pltpu.make_async_copy(sconv_h, sconv, in_sem.at[1])
    cp_snorm = pltpu.make_async_copy(snorm_h, xall.at[:, at_slot(me), :], in_sem.at[2])
    cp_text = [
        pltpu.make_async_copy(h, t_in.at[t], in_sem.at[3]) for t, h in enumerate((tk_h, tv_h))
    ]
    all_text = pltpu.make_async_copy(t_in, t_in, in_sem.at[3])
    cp_feat.start()
    cp_sconv.start()
    cp_snorm.start()
    cp_vec = [
        pltpu.make_async_copy(h, vecs.at[pl.ds(t * channels, channels)], v_sem)
        for t, h in enumerate((fg_h, fb_h, cb_h, sg_h, sb_h, lg_h))
    ]
    for c in cp_vec:
        c.start()
    row_first, row_last = chip == 0, chip == chips - 1

    @pl.when(row_first)
    def _():
        halo[0] = jnp.zeros(halo.shape[1:], BF16)
        edges[0] = jnp.zeros(edges.shape[1:], F32)

    @pl.when(row_last)
    def _():
        halo[1] = jnp.zeros(halo.shape[1:], BF16)
        edges[2] = jnp.zeros(edges.shape[1:], F32)

    for c in cp_text:
        c.start()
    cp_wc = pltpu.make_async_copy(wc_h, wc, wc_sem)
    cp_wc.start()
    cp_w = [
        pltpu.make_async_copy(h, ws.at[t], w_sem.at[t // 3])
        for t, h in enumerate((wk_h, wv_h, wq_h, wo_h, wcq_h, wco_h))
    ]

    def wait_weights(part):
        ref = ws.at[pl.ds(3 * part, 3)]
        pltpu.make_async_copy(ref, ref, w_sem.at[part]).wait()

    for c in cp_w:
        c.start()

    gather_groups = group_matrix(channels, False)
    spread_groups = group_matrix(channels, True)
    count = float(patches * cols * (channels // GROUPS))

    def local_stats(phase, x):
        sums = [jnp.sum(x[b * cols:(b + 1) * cols], axis=0, keepdims=True) for b in range(images)]
        squares = [
            jnp.sum(x[b * cols:(b + 1) * cols] * x[b * cols:(b + 1) * cols], axis=0, keepdims=True)
            for b in range(images)
        ]
        table = jnp.concatenate(sums + squares, axis=0)
        stats[phase, me] = split_dot(table, gather_groups)

    def stat_copy(phase, ref, target):
        return pltpu.make_async_remote_copy(
            src_ref=ref, dst_ref=ref, send_sem=st_send.at[phase], recv_sem=st_recv.at[phase],
            device_id={"patch": target}, device_id_type=MESH,
        )

    def send_stats(phase, wanted=None):
        def body(d, carry):
            target = lax.rem(me + d, patches)

            def send():
                stat_copy(phase, stats.at[phase, me], target).start()

            if wanted is None:
                send()
            else:
                pl.when(wanted(target // 4))(send)
            return carry
        lax.fori_loop(1, patches, body, 0)

    def all_stats(phase):
        return stat_copy(phase, stats.at[phase, pl.ds(0, patches - 1)], partner)

    def finish_stats(phase):
        all_stats(phase).wait_recv()
        total = jnp.sum(stats[phase], axis=0) / count
        mean = total[:images]
        var = total[images:] - mean * mean
        table = jnp.concatenate([mean, lax.rsqrt(var + EPSILON)], axis=0)
        return split_dot(table, spread_groups)

    def normed(x, table, b, gain, bias):
        part = x[b * cols:(b + 1) * cols]
        return (part - table[b:b + 1]) * table[images + b:images + b + 1] * gain + bias

    def x_copy(b, z, y, target, send):
        ref = xall.at[b, at_slot(index(z, y, core)), :]
        return pltpu.make_async_remote_copy(
            src_ref=ref, dst_ref=ref, send_sem=send, recv_sem=x_recv.at[b, z * 2 + y],
            device_id={"patch": target}, device_id_type=MESH,
        )

    def kv_copy(ref, which):
        return pltpu.make_async_remote_copy(
            src_ref=ref, dst_ref=ref, send_sem=kv_send.at[which], recv_sem=kv_recv,
            device_id={"patch": partner}, device_id_type=MESH,
        )

    def halo_copy(which, step):
        return pltpu.make_async_remote_copy(
            src_ref=sconv, dst_ref=halo.at[which], send_sem=halo_send.at[which],
            recv_sem=halo_recv.at[which],
            device_id={"patch": lax.rem(me + 2 * step + patches, patches)}, device_id_type=MESH,
        )

    def edge_copy(which, step):
        return pltpu.make_async_remote_copy(
            src_ref=edge_src, dst_ref=edges.at[which], send_sem=edge_send.at[which],
            recv_sem=edge_recv.at[which],
            device_id={"patch": lax.rem(partner + 2 * step + patches, patches)}, device_id_type=MESH,
        )

    mark("stats0")
    cp_feat.wait()
    x = feat[...].reshape(rows, channels).astype(F32)
    local_stats(0, x)
    mark("edges")
    cp_sconv.wait()
    whole_conv = sconv[...].astype(F32)
    edge_src[...] = jnp.where(core == 0, whole_conv[:, cols - 1], whole_conv[:, 0])
    pltpu.make_async_copy(vecs, vecs, v_sem).wait()
    vec = [vecs[pl.ds(t * channels, channels)].reshape(1, channels) for t in range(6)]
    cp_snorm.wait()

    def near(distance, visit):
        @pl.when(zo + distance < outer)
        def _():
            visit(zo + distance, 0)

        @pl.when(zo - distance >= 0)
        def _():
            visit(zo - distance, 1)

    def send_to(z):
        for b in range(images):
            x_copy(b, zo, yi, index(z, yi, core), xz_send).start()

    def send_far(first, last):
        def body(step, carry):
            near(last - step, lambda z, way: send_known(z))
            return carry

        def send_known(z):
            @pl.when(((zo >= hub) | (z < zo + 2)) & ((zo != 1) | (z != 0)))
            def _():
                send_to(z)

        lax.fori_loop(0, last - first + 1, body, 0)

    mark("barrier")
    pl.semaphore_wait(barrier, expected)
    mark("sends")

    def tell(z, carry):
        pl.semaphore_signal(
            ready, inc=1, device_id={"patch": index(z, yi, core)}, device_id_type=MESH
        )
        return carry

    @pl.when(zo == hub)
    def _():
        lax.fori_loop(0, hub, tell, 0)

    send_stats(0, lambda z: (zo >= hub) | (z <= zo))
    edge_copy(1, 0).start()

    @pl.when(yi == 0)
    def _():
        edge_copy(0, 1).start()
        halo_copy(0, 1).start()

    @pl.when(yi == 1)
    def _():
        edge_copy(2, -1).start()
        halo_copy(1, -1).start()

    for b in range(images):
        x_copy(b, zo, yi, index(zo, other, core), xy_send).start()
    if outer > 3:
        send_far(3, outer - 1)

    @pl.when(zo == 1)
    def _():
        send_to(0)

    @pl.when((yi == 0) & jnp.logical_not(row_first))
    def _():
        edge_copy(2, -1).start()
        halo_copy(1, -1).start()

    send_far(1, min(2, outer - 1))
    mark("ready")

    @pl.when(early)
    def _():
        pl.semaphore_wait(ready, 1)
        send_stats(0, lambda z: z > zo)

        @pl.when(yi == 1)
        def _():
            edge_copy(0, 1).start()
            halo_copy(0, 1).start()

        def late(step, carry):
            send_to(outer - 1 - step)
            return carry

        lax.fori_loop(0, outer - 2 - zo, late, 0)

    def wait_x(b, z, y):
        x_copy(b, z, y, partner, xy_send).wait_recv()

    around = outer - 3
    sends_around = (zo == around) & (yi == 0)
    saved = (zo == outer - 1) & (yi == 1) & (around >= 0)

    def pass_y(z):
        for b in range(images):
            wait_x(b, z, yi)

            @pl.when(jnp.logical_not(saved & (z == around)))
            def _():
                x_copy(b, z, yi, index(zo, other, core), xy_send).start()

    def distance_at(step):
        return jnp.where(zo < outer // 2, outer - step, step)

    def each_far(visit):
        def body(step, carry):
            def one(z, way):
                @pl.when(z != first)
                def _():
                    visit(z)
            near(distance_at(step), one)
            return carry
        return body

    def stale_kv(z, sides=(0, 1)):
        places = [(b, at_slot(index(z, y, core))) for b in range(images) for y in sides]
        block = jnp.concatenate([xall[b, at, :] for b, at in places], axis=0)
        for w in range(2):
            made = dot(block, ws[w]).astype(BF16)
            for t, (b, at) in enumerate(places):
                kv[w, b, at, :] = made[t * cols:(t + 1) * cols]

    def push_kv(z, sides=(0, 1)):
        for y in sides:
            at = at_slot(index(z, y, core))
            ref = kv.at[:, :, at, :]

            @pl.when((z == zo) & (yi == y))
            def _():
                kv_copy(ref, 0).start()

            @pl.when((z != zo) | (yi != y))
            def _():
                kv_copy(ref, 1).start()

    def row_taps(i, first=False):
        for j in range(3):
            made = dot(lhs[i], wc[i, j])
            taps[j] = made if first else taps[j] + made

    def fill_row(i, cells):
        for b in range(images):
            lhs[i, b * cols:(b + 1) * cols, :] = cells[b]
        filler = jnp.zeros((lhs.shape[1] - rows - images, channels), F32)
        lhs[i, rows:, :] = jnp.concatenate([edges[i], filler], axis=0).astype(BF16)

    mark("pass0")
    pass_y(first)
    mark("text")
    all_text.wait()
    for b in range(images):
        tk[b] = t_in[0, :, b, :]
        tv[b] = t_in[1, :, b, :]

    def outside(beside):
        mark("halo%d" % beside)
        below = (yi == 0) if beside else (yi == 1)
        which = jnp.where(below, 1, 0)
        row = 2 * which

        @pl.when(below & jnp.logical_not(row_last))
        def _():
            halo_copy(1, -1).wait_recv()
            edge_copy(2, -1).wait_recv()

        @pl.when(jnp.logical_not(below) & jnp.logical_not(row_first))
        def _():
            halo_copy(0, 1).wait_recv()
            edge_copy(0, 1).wait_recv()

        mark("conv%d" % beside)
        fill_row(row, halo[which])
        row_taps(row, beside)

    cp_wc.wait()
    outside(True)

    @pl.when(sends_around)
    def _():
        for b in range(images):
            wait_x(b, zo, other)
            x_copy(b, zo, other, index(outer - 1, yi, core), around_send).start()

    pass_far = each_far(pass_y)
    mark("wait0")
    table = finish_stats(0)
    mark("norm0")
    edge_copy(1, 0).wait_recv()
    centre = []
    for b in range(images):
        v = normed(x, table, b, vec[0], vec[1])
        centre.append((v * (1.0 / (1.0 + jnp.exp(-v)))).astype(BF16))
    fill_row(1, centre)
    mark("conv1")
    row_taps(1)
    mark("pass1b")
    done = jnp.where((zo == outer - 2) & (yi == 0), outer, 2)
    done = jnp.where((zo < outer // 2) | (yi == 0) & (zo == outer - 2), done, 1)
    lax.fori_loop(1, done, pass_far, 0)
    outside(False)
    mark("shift")
    place = lax.broadcasted_iota(jnp.int32, (cols, channels), 0)
    parts = []
    for b in range(images):
        at = slice(b * cols, (b + 1) * cols)
        left = pltpu.roll(taps[0, at], 1, 0)
        right = pltpu.roll(taps[2, at], cols - 1, 0)
        left_edge = jnp.where(core == 1, taps[0, rows + b:rows + b + 1], 0.0)
        right_edge = jnp.where(core == 0, taps[2, rows + b:rows + b + 1], 0.0)
        left = jnp.where(place == 0, left_edge, left)
        right = jnp.where(place == cols - 1, right_edge, right)
        conv = left + taps[1, at] + right
        parts.append(x[at] + conv + vec[2])
    hidden = jnp.concatenate(parts, axis=0)
    mark("stats1")
    local_stats(1, hidden)
    mark("send1")
    send_stats(1)
    mark("kv_own")
    wait_weights(0)

    @pl.when(jnp.logical_not(sends_around))
    def _():
        for b in range(images):
            wait_x(b, zo, other)

    stale_kv(zo)
    push_kv(zo)
    mark("pass2")
    lax.fori_loop(done, outer, pass_far, 0)

    def layer_kv(z):
        for b in range(images):
            wait_x(b, z, other)
        stale_kv(z)
        push_kv(z)

    mark("kv_first")
    layer_kv(first)

    def near_half(z):
        stale_kv(z, (yi,))
        push_kv(z, (yi,))

    def far_half(z):
        for b in range(images):
            wait_x(b, z, other)
        stale_kv(z, (other,))
        push_kv(z, (other,))

    mark("kv_far")
    lax.fori_loop(1, outer, each_far(near_half), 0)
    lax.fori_loop(1, outer, each_far(far_half), 0)
    mark("wait1")
    table = finish_stats(1)
    mark("norm1")
    attn_in = jnp.concatenate(
        [normed(hidden, table, b, vec[3], vec[4]) for b in range(images)], axis=0
    ).astype(BF16)
    own = at_slot(me)
    kv_copy(kv.at[:, :, own, :], 0).wait_send()
    for w in range(2):
        fresh = dot(attn_in, ws[w]).astype(BF16)
        for b in range(images):
            kv[w, b, own, :] = fresh[b * cols:(b + 1) * cols]
    mark("q")
    scale = HEAD_DIM ** -0.5
    lane = lax.broadcasted_iota(jnp.int32, (cols, LANES), 1)
    pairs = channels // LANES

    def heads(q, keys, values, together):
        for first in range(0, images, together):
            places = [
                (b, slice(p * LANES, (p + 1) * LANES))
                for b in range(first, first + together) for p in range(pairs)
            ]
            units = [
                (q[b * cols:(b + 1) * cols, at], keys[b, :, at], values[b, :, at])
                for b, at in places
            ]
            for (b, at), part in zip(places, attention_stages(units, lane)):
                att[b * cols:(b + 1) * cols, at] = part.astype(BF16)

    query = dot(attn_in, ws[2]).astype(BF16).astype(F32) * scale
    mark("kvwait")
    kv_copy(kv.at[0], 1).wait_recv()
    mark("attend")
    heads(query, kv.at[0], kv.at[1], images)
    mark("out_ln")
    wait_weights(1)
    mixed = hidden + dot(att[...], ws[3])
    centred = mixed - jnp.mean(mixed, axis=-1, keepdims=True)
    variance = jnp.mean(centred * centred, axis=-1, keepdims=True)
    layer_in = (centred * lax.rsqrt(variance + EPSILON) * vec[5]).astype(BF16)
    mark("cross")
    heads(dot(layer_in, ws[4]).astype(BF16).astype(F32) * scale, tk, tv, images)
    mark("out")
    out_ref[...] = mixed + dot(att[...], ws[5])

    mark("drain")
    all_stats(0).wait_send()
    all_stats(1).wait_send()
    def sent(blocks, send):
        for b in range(images):
            ref = xall.at[b, pl.ds(0, blocks * cols), :]
            pltpu.make_async_remote_copy(
                src_ref=ref, dst_ref=ref, send_sem=send, recv_sem=x_recv.at[0, 0],
                device_id={"patch": partner}, device_id_type=MESH,
            ).wait_send()

    sent(outer - 1, xz_send)


    @pl.when(saved)
    def _():
        sent(outer - 1, xy_send)

    @pl.when(jnp.logical_not(saved))
    def _():
        sent(outer, xy_send)

    @pl.when(sends_around)
    def _():
        sent(1, around_send)

    kv_copy(kv.at[0, :, pl.ds(0, (patches - 2) * cols)], 1).wait_send()
    edge_copy(1, 0).wait_send()

    @pl.when(jnp.logical_not(row_last))
    def _():
        halo_copy(0, 1).wait_send()
        edge_copy(0, 1).wait_send()

    @pl.when(jnp.logical_not(row_first))
    def _():
        halo_copy(1, -1).wait_send()
        edge_copy(2, -1).wait_send()


def solution(mesh):
    patches = mesh.shape["patch"]

    def on_device(
        features, stale_conv_in, stale_normed, first_gain, first_bias, conv_weight, conv_bias,
        second_gain, second_bias, query_weight, key_weight, value_weight, output_weight,
        layer_gain, cross_query, cross_output, text_keys, text_values,
    ):
        images, _, cols, channels = features.shape
        rows = images * cols
        span = patches * cols
        outer = patches // 4
        ctx = text_keys.shape[1]

        def flat(a):
            return a.reshape(images, cols, channels)

        dma = pltpu.SemaphoreType.DMA
        out = pl.pallas_call(
            functools.partial(kernel, patches, images, cols),
            out_shape=pltpu.VMEM((rows, channels), F32),
            in_specs=[pl.BlockSpec(memory_space=pltpu.HBM)] * 18,
            out_specs=pl.BlockSpec(memory_space=pltpu.VMEM),
            scratch_shapes=[
                pltpu.VMEM((images, cols, channels), BF16),
                pltpu.VMEM((images, cols, channels), BF16),
                pltpu.VMEM((images, span, channels), BF16),
                pltpu.VMEM((2, images, span, channels), BF16),
                pltpu.VMEM(conv_weight.shape, BF16),
                pltpu.VMEM((6, channels, channels), BF16),
                pltpu.VMEM((6 * channels,), F32),
                pltpu.VMEM((2, ctx, images, channels), BF16),
                pltpu.VMEM((images, ctx, channels), BF16),
                pltpu.VMEM((images, ctx, channels), BF16),
                pltpu.VMEM((2, patches, 2 * images, LANES), F32),
                pltpu.VMEM((2, images, cols, channels), BF16),
                pltpu.VMEM((images, channels), F32),
                pltpu.VMEM((3, images, channels), F32),
                pltpu.VMEM((3, rows + 16, channels), BF16),
                pltpu.VMEM((3, rows + 16, channels), F32),
                pltpu.VMEM((rows, channels), BF16),
                dma((2,)), dma((2,)), dma, dma, dma,
                dma((images, 2 * outer)), dma((2,)), dma,
                dma((2,)), dma((2,)), dma((3,)), dma((3,)), pltpu.SemaphoreType.REGULAR,
                dma((4,)), dma, dma((2,)), dma,
            ],
            compiler_params=pltpu.CompilerParams(
                collective_id=0, has_side_effects=True, vmem_limit_bytes=60000 * 1024
            ),
        )(
            flat(features), flat(stale_conv_in), flat(stale_normed), first_gain, first_bias,
            conv_weight, conv_bias, second_gain, second_bias, query_weight, key_weight,
            value_weight, output_weight, layer_gain, cross_query, cross_output,
            text_keys.transpose(1, 0, 2), text_values.transpose(1, 0, 2),
        )
        return out.reshape(features.shape)

    act = P("grp", "patch", None, None)
    text = P("grp", None, None)
    return jax.shard_map(
        on_device, mesh=mesh,
        in_specs=(act,) * 3 + (P(),) * 13 + (text,) * 2,
        out_specs=act, check_vma=False,
    )
```

```python
import functools

import jax
import jax.numpy as jnp
from jax import lax
from jax.experimental import pallas as pl
from jax.experimental.pallas import tpu as pltpu
from jax.sharding import PartitionSpec as P

GROUPS = 32
HEADS = 10
HEAD_DIM = 64
EPSILON = 1e-05
MESH = pl.DeviceIdType.MESH
LANES = 128
F32 = jnp.float32
BF16 = jnp.bfloat16


def mark(name):
    pass


def dot(a, b, **kw):
    return jnp.dot(a, b, preferred_element_type=F32, **kw)


def dot_t(a, b):
    return lax.dot_general(a, b, (((1,), (1,)), ((), ())), preferred_element_type=F32)


def group_matrix(channels, transposed):
    width = channels // GROUPS
    shape = (LANES, channels) if transposed else (channels, LANES)
    channel = lax.broadcasted_iota(jnp.int32, shape, 1 if transposed else 0)
    group = lax.broadcasted_iota(jnp.int32, shape, 0 if transposed else 1)
    inside = (channel >= group * width) & (channel < (group + 1) * width)
    return jnp.where(inside, 1.0, 0.0).astype(BF16)


def split_dot(x, selector):
    high = x.astype(BF16)
    rest = x - high.astype(F32)
    middle = rest.astype(BF16)
    low = (rest - middle.astype(F32)).astype(BF16)
    made = dot(jnp.concatenate([high, middle, low], axis=0), selector)
    n = x.shape[0]
    return made[:n] + made[n:2 * n] + made[2 * n:]


def attention_stages(units, lane):
    low = lane < HEAD_DIM
    scores = []
    for q, k, _ in units:
        both = jnp.concatenate([jnp.where(low, q, 0.0), jnp.where(low, 0.0, q)], axis=0)
        scores.append(dot_t(both.astype(BF16), k))
    weights = [jnp.exp(s - jnp.max(s, axis=-1, keepdims=True)) for s in scores]
    totals = [jnp.sum(w, axis=-1, keepdims=True) for w in weights]
    outs = [dot(w.astype(BF16), v) for w, (_, _, v) in zip(weights, units)]
    outs = [o / t for o, t in zip(outs, totals)]
    cols = lane.shape[0]
    return [jnp.where(low, o[:cols], o[cols:]) for o in outs]


def kernel(
    patches, images, cols,
    feat_h, sconv_h, snorm_h, fg_h, fb_h, wc_h, cb_h, sg_h, sb_h,
    wq_h, wk_h, wv_h, wo_h, lg_h, wcq_h, wco_h, tk_h, tv_h,
    out_ref,
    feat, sconv, xall, kv, wc, ws, vecs, t_in, tk, tv,
    stats, halo, edge_src, edges, lhs, taps, att,
    st_send, st_recv, xz_send, xy_send, around_send, x_recv, kv_send, kv_recv,
    halo_send, halo_recv, edge_send, edge_recv, ready, in_sem, wc_sem, w_sem, v_sem,
):
    channels = feat.shape[-1]
    rows = images * cols
    outer = patches // 4
    chips = patches // 2
    me = lax.axis_index("patch")
    chip, core = me // 2, me % 2
    zo, yi = chip // 2, chip % 2
    other = 1 - yi
    first = jnp.where(zo > 0, zo - 1, 1)
    partner = chip * 2 + (1 - core)

    def index(o, i, c):
        return (o * 2 + i) * 2 + c

    def at_slot(slot):
        return pl.ds(pl.multiple_of(slot * cols, cols), cols)

    barrier = pltpu.get_barrier_semaphore()

    hub = outer - 1
    early = zo < hub
    expected = jnp.where(early, 4 * zo + 5 + 2 * yi, patches - 1)

    def greet(d, carry):
        target = lax.rem(me + d, patches)
        tz, ty = target // 4, (target // 2) % 2
        next_up = (zo == tz + 1) & ((yi == ty) | (chip == target // 2 + 1))

        @pl.when((tz >= hub) | (zo <= tz) | next_up)
        def _():
            pl.semaphore_signal(
                barrier, inc=1, device_id={"patch": target}, device_id_type=MESH
            )
        return carry

    lax.fori_loop(1, patches, greet, 0, unroll=patches <= 16)
    cp_feat = pltpu.make_async_copy(feat_h, feat, in_sem.at[0])
    cp_sconv = pltpu.make_async_copy(sconv_h, sconv, in_sem.at[1])
    cp_snorm = pltpu.make_async_copy(snorm_h, xall.at[:, at_slot(me), :], in_sem.at[2])
    cp_text = [
        pltpu.make_async_copy(h, t_in.at[t], in_sem.at[3]) for t, h in enumerate((tk_h, tv_h))
    ]
    all_text = pltpu.make_async_copy(t_in, t_in, in_sem.at[3])
    cp_feat.start()
    cp_sconv.start()
    cp_snorm.start()
    cp_vec = [
        pltpu.make_async_copy(h, vecs.at[pl.ds(t * channels, channels)], v_sem)
        for t, h in enumerate((fg_h, fb_h, cb_h, sg_h, sb_h, lg_h))
    ]
    for c in cp_vec:
        c.start()
    row_first, row_last = chip == 0, chip == chips - 1

    @pl.when(row_first)
    def _():
        halo[0] = jnp.zeros(halo.shape[1:], BF16)
        edges[0] = jnp.zeros(edges.shape[1:], F32)

    @pl.when(row_last)
    def _():
        halo[1] = jnp.zeros(halo.shape[1:], BF16)
        edges[2] = jnp.zeros(edges.shape[1:], F32)

    for c in cp_text:
        c.start()
    cp_wc = pltpu.make_async_copy(wc_h, wc, wc_sem)
    cp_wc.start()
    cp_w = [
        pltpu.make_async_copy(h, ws.at[t], w_sem.at[t // 3])
        for t, h in enumerate((wk_h, wv_h, wq_h, wo_h, wcq_h, wco_h))
    ]

    def wait_weights(part):
        ref = ws.at[pl.ds(3 * part, 3)]
        pltpu.make_async_copy(ref, ref, w_sem.at[part]).wait()

    for c in cp_w:
        c.start()

    gather_groups = group_matrix(channels, False)
    spread_groups = group_matrix(channels, True)
    count = float(patches * cols * (channels // GROUPS))

    def local_stats(phase, x):
        sums = [jnp.sum(x[b * cols:(b + 1) * cols], axis=0, keepdims=True) for b in range(images)]
        squares = [
            jnp.sum(x[b * cols:(b + 1) * cols] * x[b * cols:(b + 1) * cols], axis=0, keepdims=True)
            for b in range(images)
        ]
        table = jnp.concatenate(sums + squares, axis=0)
        stats[phase, me] = split_dot(table, gather_groups)

    def stat_copy(phase, ref, target):
        return pltpu.make_async_remote_copy(
            src_ref=ref, dst_ref=ref, send_sem=st_send.at[phase], recv_sem=st_recv.at[phase],
            device_id={"patch": target}, device_id_type=MESH,
        )

    def send_stats(phase, wanted=None):
        def body(d, carry):
            target = lax.rem(me + d, patches)

            def send():
                stat_copy(phase, stats.at[phase, me], target).start()

            if wanted is None:
                send()
            else:
                pl.when(wanted(target // 4))(send)
            return carry
        lax.fori_loop(1, patches, body, 0, unroll=patches <= 16)

    def all_stats(phase):
        return stat_copy(phase, stats.at[phase, pl.ds(0, patches - 1)], partner)

    def finish_stats(phase):
        all_stats(phase).wait_recv()
        total = jnp.sum(stats[phase], axis=0) / count
        mean = total[:images]
        var = total[images:] - mean * mean
        table = jnp.concatenate([mean, lax.rsqrt(var + EPSILON)], axis=0)
        return split_dot(table, spread_groups)

    def normed(x, table, b, gain, bias):
        part = x[b * cols:(b + 1) * cols]
        return (part - table[b:b + 1]) * table[images + b:images + b + 1] * gain + bias

    def x_copy(b, z, y, target, send):
        ref = xall.at[b, at_slot(index(z, y, core)), :]
        return pltpu.make_async_remote_copy(
            src_ref=ref, dst_ref=ref, send_sem=send, recv_sem=x_recv.at[b, z * 2 + y],
            device_id={"patch": target}, device_id_type=MESH,
        )

    def kv_copy(ref, which):
        return pltpu.make_async_remote_copy(
            src_ref=ref, dst_ref=ref, send_sem=kv_send.at[which], recv_sem=kv_recv,
            device_id={"patch": partner}, device_id_type=MESH,
        )

    def halo_copy(which, step):
        return pltpu.make_async_remote_copy(
            src_ref=sconv, dst_ref=halo.at[which], send_sem=halo_send.at[which],
            recv_sem=halo_recv.at[which],
            device_id={"patch": lax.rem(me + 2 * step + patches, patches)}, device_id_type=MESH,
        )

    def edge_copy(which, step):
        return pltpu.make_async_remote_copy(
            src_ref=edge_src, dst_ref=edges.at[which], send_sem=edge_send.at[which],
            recv_sem=edge_recv.at[which],
            device_id={"patch": lax.rem(partner + 2 * step + patches, patches)}, device_id_type=MESH,
        )

    mark("stats0")
    cp_feat.wait()
    x = feat[...].reshape(rows, channels).astype(F32)
    local_stats(0, x)
    mark("edges")
    cp_sconv.wait()
    whole_conv = sconv[...].astype(F32)
    edge_src[...] = jnp.where(core == 0, whole_conv[:, cols - 1], whole_conv[:, 0])
    pltpu.make_async_copy(vecs, vecs, v_sem).wait()
    vec = [vecs[pl.ds(t * channels, channels)].reshape(1, channels) for t in range(6)]
    cp_snorm.wait()

    def near(distance, visit):
        @pl.when(zo + distance < outer)
        def _():
            visit(zo + distance, 0)

        @pl.when(zo - distance >= 0)
        def _():
            visit(zo - distance, 1)

    def send_to(z):
        for b in range(images):
            x_copy(b, zo, yi, index(z, yi, core), xz_send).start()

    def send_far(first, last):
        def body(step, carry):
            near(last - step, lambda z, way: send_known(z))
            return carry

        def send_known(z):
            @pl.when(((zo >= hub) | (z < zo + 2)) & ((zo != 1) | (z != 0)))
            def _():
                send_to(z)

        lax.fori_loop(0, last - first + 1, body, 0)

    mark("barrier")
    pl.semaphore_wait(barrier, expected)
    mark("sends")

    def tell(z, carry):
        pl.semaphore_signal(
            ready, inc=1, device_id={"patch": index(z, yi, core)}, device_id_type=MESH
        )
        return carry

    @pl.when(zo == hub)
    def _():
        lax.fori_loop(0, hub, tell, 0)

    send_stats(0, lambda z: (zo >= hub) | (z <= zo))
    edge_copy(1, 0).start()

    @pl.when(yi == 0)
    def _():
        edge_copy(0, 1).start()
        halo_copy(0, 1).start()

    @pl.when(yi == 1)
    def _():
        edge_copy(2, -1).start()
        halo_copy(1, -1).start()

    for b in range(images):
        x_copy(b, zo, yi, index(zo, other, core), xy_send).start()
    if outer > 3:
        send_far(3, outer - 1)

    @pl.when(zo == 1)
    def _():
        send_to(0)

    @pl.when((yi == 0) & jnp.logical_not(row_first))
    def _():
        edge_copy(2, -1).start()
        halo_copy(1, -1).start()

    send_far(1, min(2, outer - 1))
    mark("ready")

    @pl.when(early)
    def _():
        pl.semaphore_wait(ready, 1)
        send_stats(0, lambda z: z > zo)

        @pl.when(yi == 1)
        def _():
            edge_copy(0, 1).start()
            halo_copy(0, 1).start()

        def late(step, carry):
            send_to(outer - 1 - step)
            return carry

        lax.fori_loop(0, outer - 2 - zo, late, 0)

    def wait_x(b, z, y):
        x_copy(b, z, y, partner, xy_send).wait_recv()

    around = outer - 3
    sends_around = (zo == around) & (yi == 0)
    saved = (zo == outer - 1) & (yi == 1) & (around >= 0)

    def pass_y(z):
        for b in range(images):
            wait_x(b, z, yi)

            @pl.when(jnp.logical_not(saved & (z == around)))
            def _():
                x_copy(b, z, yi, index(zo, other, core), xy_send).start()

    def distance_at(step):
        return jnp.where(zo < outer // 2, outer - step, step)

    def each_far(visit):
        def body(step, carry):
            def one(z, way):
                @pl.when(z != first)
                def _():
                    visit(z)
            near(distance_at(step), one)
            return carry
        return body

    def stale_kv(z, sides=(0, 1)):
        places = [(b, at_slot(index(z, y, core))) for b in range(images) for y in sides]
        block = jnp.concatenate([xall[b, at, :] for b, at in places], axis=0)
        for w in range(2):
            made = dot(block, ws[w]).astype(BF16)
            for t, (b, at) in enumerate(places):
                kv[w, b, at, :] = made[t * cols:(t + 1) * cols]

    def push_kv(z, sides=(0, 1)):
        for y in sides:
            at = at_slot(index(z, y, core))
            ref = kv.at[:, :, at, :]

            @pl.when((z == zo) & (yi == y))
            def _():
                kv_copy(ref, 0).start()

            @pl.when((z != zo) | (yi != y))
            def _():
                kv_copy(ref, 1).start()

    def row_taps(i, first=False):
        for j in range(3):
            made = dot(lhs[i], wc[i, j])
            taps[j] = made if first else taps[j] + made

    def fill_row(i, cells):
        for b in range(images):
            lhs[i, b * cols:(b + 1) * cols, :] = cells[b]
        filler = jnp.zeros((lhs.shape[1] - rows - images, channels), F32)
        lhs[i, rows:, :] = jnp.concatenate([edges[i], filler], axis=0).astype(BF16)

    mark("pass0")
    pass_y(first)
    mark("text")
    all_text.wait()
    for b in range(images):
        tk[b] = t_in[0, :, b, :]
        tv[b] = t_in[1, :, b, :]

    def outside(beside):
        mark("halo%d" % beside)
        below = (yi == 0) if beside else (yi == 1)
        which = jnp.where(below, 1, 0)
        row = 2 * which

        @pl.when(below & jnp.logical_not(row_last))
        def _():
            halo_copy(1, -1).wait_recv()
            edge_copy(2, -1).wait_recv()

        @pl.when(jnp.logical_not(below) & jnp.logical_not(row_first))
        def _():
            halo_copy(0, 1).wait_recv()
            edge_copy(0, 1).wait_recv()

        mark("conv%d" % beside)
        fill_row(row, halo[which])
        row_taps(row, beside)

    cp_wc.wait()
    outside(True)

    @pl.when(sends_around)
    def _():
        for b in range(images):
            wait_x(b, zo, other)
            x_copy(b, zo, other, index(outer - 1, yi, core), around_send).start()

    pass_far = each_far(pass_y)
    mark("wait0")
    table = finish_stats(0)
    mark("norm0")
    edge_copy(1, 0).wait_recv()
    centre = []
    for b in range(images):
        v = normed(x, table, b, vec[0], vec[1])
        centre.append((v * (1.0 / (1.0 + jnp.exp(-v)))).astype(BF16))
    fill_row(1, centre)
    mark("conv1")
    row_taps(1)
    mark("pass1b")
    done = jnp.where((zo == outer - 2) & (yi == 0), outer, 2)
    done = jnp.where((zo < outer // 2) | (yi == 0) & (zo == outer - 2), done, 1)
    lax.fori_loop(1, done, pass_far, 0)
    outside(False)
    mark("shift")
    place = lax.broadcasted_iota(jnp.int32, (cols, channels), 0)
    parts = []
    for b in range(images):
        at = slice(b * cols, (b + 1) * cols)
        left = pltpu.roll(taps[0, at], 1, 0)
        right = pltpu.roll(taps[2, at], cols - 1, 0)
        left_edge = jnp.where(core == 1, taps[0, rows + b:rows + b + 1], 0.0)
        right_edge = jnp.where(core == 0, taps[2, rows + b:rows + b + 1], 0.0)
        left = jnp.where(place == 0, left_edge, left)
        right = jnp.where(place == cols - 1, right_edge, right)
        conv = left + taps[1, at] + right
        parts.append(x[at] + conv + vec[2])
    hidden = jnp.concatenate(parts, axis=0)
    mark("stats1")
    local_stats(1, hidden)
    mark("send1")
    send_stats(1)
    mark("kv_own")
    wait_weights(0)

    @pl.when(jnp.logical_not(sends_around))
    def _():
        for b in range(images):
            wait_x(b, zo, other)

    stale_kv(zo)
    push_kv(zo)
    mark("pass2")
    lax.fori_loop(done, outer, pass_far, 0)

    def layer_kv(z):
        for b in range(images):
            wait_x(b, z, other)
        stale_kv(z)
        push_kv(z)

    mark("kv_first")
    layer_kv(first)

    def near_half(z):
        stale_kv(z, (yi,))
        push_kv(z, (yi,))

    def far_half(z):
        for b in range(images):
            wait_x(b, z, other)
        stale_kv(z, (other,))
        push_kv(z, (other,))

    mark("kv_far")
    lax.fori_loop(1, outer, each_far(near_half), 0)
    lax.fori_loop(1, outer, each_far(far_half), 0)
    mark("kvwait")
    own = at_slot(me)
    kv_copy(kv.at[:, :, own, :], 0).wait_send()
    kv_copy(kv.at[0], 1).wait_recv()
    wait_weights(1)
    mark("wait1")
    table = finish_stats(1)
    mark("norm1")
    attn_in = jnp.concatenate(
        [normed(hidden, table, b, vec[3], vec[4]) for b in range(images)], axis=0
    ).astype(BF16)
    for w in range(2):
        fresh = dot(attn_in, ws[w]).astype(BF16)
        for b in range(images):
            kv[w, b, own, :] = fresh[b * cols:(b + 1) * cols]
    mark("q")
    scale = HEAD_DIM ** -0.5
    lane = lax.broadcasted_iota(jnp.int32, (cols, LANES), 1)
    pairs = channels // LANES

    def heads(q, keys, values, together):
        for first in range(0, images, together):
            places = [
                (b, slice(p * LANES, (p + 1) * LANES))
                for b in range(first, first + together) for p in range(pairs)
            ]
            units = [
                (q[b * cols:(b + 1) * cols, at], keys[b, :, at], values[b, :, at])
                for b, at in places
            ]
            for (b, at), part in zip(places, attention_stages(units, lane)):
                att[b * cols:(b + 1) * cols, at] = part.astype(BF16)

    query = dot(attn_in, ws[2]).astype(BF16).astype(F32) * scale
    mark("attend")
    heads(query, kv.at[0], kv.at[1], images)
    mark("out_ln")
    mixed = hidden + dot(att[...], ws[3])
    centred = mixed - jnp.mean(mixed, axis=-1, keepdims=True)
    variance = jnp.mean(centred * centred, axis=-1, keepdims=True)
    layer_in = (centred * lax.rsqrt(variance + EPSILON) * vec[5]).astype(BF16)
    mark("cross")
    heads(dot(layer_in, ws[4]).astype(BF16).astype(F32) * scale, tk, tv, images)
    mark("out")
    out_ref[...] = mixed + dot(att[...], ws[5])

    mark("drain")
    all_stats(0).wait_send()
    all_stats(1).wait_send()
    def sent(blocks, send):
        for b in range(images):
            ref = xall.at[b, pl.ds(0, blocks * cols), :]
            pltpu.make_async_remote_copy(
                src_ref=ref, dst_ref=ref, send_sem=send, recv_sem=x_recv.at[0, 0],
                device_id={"patch": partner}, device_id_type=MESH,
            ).wait_send()

    sent(outer - 1, xz_send)


    @pl.when(saved)
    def _():
        sent(outer - 1, xy_send)

    @pl.when(jnp.logical_not(saved))
    def _():
        sent(outer, xy_send)

    @pl.when(sends_around)
    def _():
        sent(1, around_send)

    kv_copy(kv.at[0, :, pl.ds(0, (patches - 2) * cols)], 1).wait_send()
    edge_copy(1, 0).wait_send()

    @pl.when(jnp.logical_not(row_last))
    def _():
        halo_copy(0, 1).wait_send()
        edge_copy(0, 1).wait_send()

    @pl.when(jnp.logical_not(row_first))
    def _():
        halo_copy(1, -1).wait_send()
        edge_copy(2, -1).wait_send()


def solution(mesh):
    patches = mesh.shape["patch"]

    def on_device(
        features, stale_conv_in, stale_normed, first_gain, first_bias, conv_weight, conv_bias,
        second_gain, second_bias, query_weight, key_weight, value_weight, output_weight,
        layer_gain, cross_query, cross_output, text_keys, text_values,
    ):
        images, _, cols, channels = features.shape
        rows = images * cols
        span = patches * cols
        outer = patches // 4
        ctx = text_keys.shape[1]

        def flat(a):
            return a.reshape(images, cols, channels)

        dma = pltpu.SemaphoreType.DMA
        out = pl.pallas_call(
            functools.partial(kernel, patches, images, cols),
            out_shape=pltpu.VMEM((rows, channels), F32),
            in_specs=[pl.BlockSpec(memory_space=pltpu.HBM)] * 18,
            out_specs=pl.BlockSpec(memory_space=pltpu.VMEM),
            scratch_shapes=[
                pltpu.VMEM((images, cols, channels), BF16),
                pltpu.VMEM((images, cols, channels), BF16),
                pltpu.VMEM((images, span, channels), BF16),
                pltpu.VMEM((2, images, span, channels), BF16),
                pltpu.VMEM(conv_weight.shape, BF16),
                pltpu.VMEM((6, channels, channels), BF16),
                pltpu.VMEM((6 * channels,), F32),
                pltpu.VMEM((2, ctx, images, channels), BF16),
                pltpu.VMEM((images, ctx, channels), BF16),
                pltpu.VMEM((images, ctx, channels), BF16),
                pltpu.VMEM((2, patches, 2 * images, LANES), F32),
                pltpu.VMEM((2, images, cols, channels), BF16),
                pltpu.VMEM((images, channels), F32),
                pltpu.VMEM((3, images, channels), F32),
                pltpu.VMEM((3, rows + 16, channels), BF16),
                pltpu.VMEM((3, rows + 16, channels), F32),
                pltpu.VMEM((rows, channels), BF16),
                dma((2,)), dma((2,)), dma, dma, dma,
                dma((images, 2 * outer)), dma((2,)), dma,
                dma((2,)), dma((2,)), dma((3,)), dma((3,)), pltpu.SemaphoreType.REGULAR,
                dma((4,)), dma, dma((2,)), dma,
            ],
            compiler_params=pltpu.CompilerParams(
                collective_id=0, has_side_effects=True, vmem_limit_bytes=60000 * 1024
            ),
        )(
            flat(features), flat(stale_conv_in), flat(stale_normed), first_gain, first_bias,
            conv_weight, conv_bias, second_gain, second_bias, query_weight, key_weight,
            value_weight, output_weight, layer_gain, cross_query, cross_output,
            text_keys.transpose(1, 0, 2), text_values.transpose(1, 0, 2),
        )
        return out.reshape(features.shape)

    act = P("grp", "patch", None, None)
    text = P("grp", None, None)
    return jax.shard_map(
        on_device, mesh=mesh,
        in_specs=(act,) * 3 + (P(),) * 13 + (text,) * 2,
        out_specs=act, check_vma=False,
    )
```

```python
import functools

import jax
import jax.numpy as jnp
from jax import lax
from jax.experimental import pallas as pl
from jax.experimental.pallas import tpu as pltpu
from jax.sharding import PartitionSpec as P

GROUPS = 32
HEADS = 10
HEAD_DIM = 64
EPSILON = 1e-05
MESH = pl.DeviceIdType.MESH
LANES = 128
F32 = jnp.float32
BF16 = jnp.bfloat16


def mark(name):
    pass


def dot(a, b, **kw):
    return jnp.dot(a, b, preferred_element_type=F32, **kw)


def dot_t(a, b):
    return lax.dot_general(a, b, (((1,), (1,)), ((), ())), preferred_element_type=F32)


def group_matrix(channels, transposed):
    width = channels // GROUPS
    shape = (LANES, channels) if transposed else (channels, LANES)
    channel = lax.broadcasted_iota(jnp.int32, shape, 1 if transposed else 0)
    group = lax.broadcasted_iota(jnp.int32, shape, 0 if transposed else 1)
    inside = (channel >= group * width) & (channel < (group + 1) * width)
    return jnp.where(inside, 1.0, 0.0).astype(BF16)


def split_dot(x, selector):
    high = x.astype(BF16)
    rest = x - high.astype(F32)
    middle = rest.astype(BF16)
    low = (rest - middle.astype(F32)).astype(BF16)
    made = dot(jnp.concatenate([high, middle, low], axis=0), selector)
    n = x.shape[0]
    return made[:n] + made[n:2 * n] + made[2 * n:]


def attention_stages(units, lane):
    low = lane < HEAD_DIM
    scores = []
    for q, k, _ in units:
        both = jnp.concatenate([jnp.where(low, q, 0.0), jnp.where(low, 0.0, q)], axis=0)
        scores.append(dot_t(both.astype(BF16), k))
    weights = [jnp.exp(s - jnp.max(s, axis=-1, keepdims=True)) for s in scores]
    totals = [jnp.sum(w, axis=-1, keepdims=True) for w in weights]
    outs = [dot(w.astype(BF16), v) for w, (_, _, v) in zip(weights, units)]
    outs = [o / t for o, t in zip(outs, totals)]
    cols = lane.shape[0]
    return [jnp.where(low, o[:cols], o[cols:]) for o in outs]


def kernel(
    patches, images, cols,
    feat_h, sconv_h, snorm_h, fg_h, fb_h, wc_h, cb_h, sg_h, sb_h,
    wq_h, wk_h, wv_h, wo_h, lg_h, wcq_h, wco_h, tk_h, tv_h,
    out_ref,
    feat, sconv, xall, kv, wc, ws, vecs, t_in, tk, tv,
    stats, halo, edge_src, edges, lhs, taps, att,
    st_send, st_recv, xz_send, xy_send, around_send, x_recv, kv_send, kv_recv,
    halo_send, halo_recv, edge_send, edge_recv, ready, in_sem, wc_sem, w_sem, v_sem,
):
    channels = feat.shape[-1]
    rows = images * cols
    outer = patches // 4
    chips = patches // 2
    me = lax.axis_index("patch")
    chip, core = me // 2, me % 2
    zo, yi = chip // 2, chip % 2
    other = 1 - yi
    first = jnp.where(zo > 0, zo - 1, 1)
    partner = chip * 2 + (1 - core)

    def index(o, i, c):
        return (o * 2 + i) * 2 + c

    def at_slot(slot):
        return pl.ds(pl.multiple_of(slot * cols, cols), cols)

    barrier = pltpu.get_barrier_semaphore()

    hub = outer - 1
    early = zo < hub
    expected = jnp.where(early, 4 * zo + 5 + 2 * yi, patches - 1)

    def greet(d, carry):
        target = lax.rem(me + d, patches)
        tz, ty = target // 4, (target // 2) % 2
        next_up = (zo == tz + 1) & ((yi == ty) | (chip == target // 2 + 1))

        @pl.when((tz >= hub) | (zo <= tz) | next_up)
        def _():
            pl.semaphore_signal(
                barrier, inc=1, device_id={"patch": target}, device_id_type=MESH
            )
        return carry

    lax.fori_loop(1, patches, greet, 0, unroll=patches <= 16)
    cp_feat = pltpu.make_async_copy(feat_h, feat, in_sem.at[0])
    cp_sconv = pltpu.make_async_copy(sconv_h, sconv, in_sem.at[1])
    cp_snorm = pltpu.make_async_copy(snorm_h, xall.at[:, at_slot(me), :], in_sem.at[2])
    cp_text = [
        pltpu.make_async_copy(h, t_in.at[t], in_sem.at[3]) for t, h in enumerate((tk_h, tv_h))
    ]
    all_text = pltpu.make_async_copy(t_in, t_in, in_sem.at[3])
    cp_feat.start()
    cp_sconv.start()
    cp_snorm.start()
    cp_vec = [
        pltpu.make_async_copy(h, vecs.at[pl.ds(t * channels, channels)], v_sem)
        for t, h in enumerate((fg_h, fb_h, cb_h, sg_h, sb_h, lg_h))
    ]
    for c in cp_vec:
        c.start()
    row_first, row_last = chip == 0, chip == chips - 1

    @pl.when(row_first)
    def _():
        halo[0] = jnp.zeros(halo.shape[1:], BF16)
        edges[0] = jnp.zeros(edges.shape[1:], F32)

    @pl.when(row_last)
    def _():
        halo[1] = jnp.zeros(halo.shape[1:], BF16)
        edges[2] = jnp.zeros(edges.shape[1:], F32)

    for c in cp_text:
        c.start()
    cp_wc = pltpu.make_async_copy(wc_h, wc, wc_sem)
    cp_wc.start()
    cp_w = [
        pltpu.make_async_copy(h, ws.at[t], w_sem.at[t // 3])
        for t, h in enumerate((wk_h, wv_h, wq_h, wo_h, wcq_h, wco_h))
    ]

    def wait_weights(part):
        ref = ws.at[pl.ds(3 * part, 3)]
        pltpu.make_async_copy(ref, ref, w_sem.at[part]).wait()

    for c in cp_w:
        c.start()

    gather_groups = group_matrix(channels, False)
    spread_groups = group_matrix(channels, True)
    count = float(patches * cols * (channels // GROUPS))

    def local_stats(phase, x):
        sums = [jnp.sum(x[b * cols:(b + 1) * cols], axis=0, keepdims=True) for b in range(images)]
        squares = [
            jnp.sum(x[b * cols:(b + 1) * cols] * x[b * cols:(b + 1) * cols], axis=0, keepdims=True)
            for b in range(images)
        ]
        table = jnp.concatenate(sums + squares, axis=0)
        stats[phase, me] = split_dot(table, gather_groups)

    def stat_copy(phase, ref, target):
        return pltpu.make_async_remote_copy(
            src_ref=ref, dst_ref=ref, send_sem=st_send.at[phase], recv_sem=st_recv.at[phase],
            device_id={"patch": target}, device_id_type=MESH,
        )

    def send_stats(phase, wanted=None):
        def body(d, carry):
            target = lax.rem(me + d, patches)

            def send():
                stat_copy(phase, stats.at[phase, me], target).start()

            if wanted is None:
                send()
            else:
                pl.when(wanted(target // 4))(send)
            return carry
        lax.fori_loop(1, patches, body, 0, unroll=patches <= 16)

    def all_stats(phase):
        return stat_copy(phase, stats.at[phase, pl.ds(0, patches - 1)], partner)

    def finish_stats(phase):
        all_stats(phase).wait_recv()
        total = jnp.sum(stats[phase], axis=0) / count
        mean = total[:images]
        var = total[images:] - mean * mean
        table = jnp.concatenate([mean, lax.rsqrt(var + EPSILON)], axis=0)
        return split_dot(table, spread_groups)

    def normed(x, table, b, gain, bias):
        part = x[b * cols:(b + 1) * cols]
        return (part - table[b:b + 1]) * table[images + b:images + b + 1] * gain + bias

    def x_copy(b, z, y, target, send):
        ref = xall.at[b, at_slot(index(z, y, core)), :]
        return pltpu.make_async_remote_copy(
            src_ref=ref, dst_ref=ref, send_sem=send, recv_sem=x_recv.at[b, z * 2 + y],
            device_id={"patch": target}, device_id_type=MESH,
        )

    def kv_copy(ref, which):
        return pltpu.make_async_remote_copy(
            src_ref=ref, dst_ref=ref, send_sem=kv_send.at[which], recv_sem=kv_recv,
            device_id={"patch": partner}, device_id_type=MESH,
        )

    def halo_copy(which, step):
        return pltpu.make_async_remote_copy(
            src_ref=sconv, dst_ref=halo.at[which], send_sem=halo_send.at[which],
            recv_sem=halo_recv.at[which],
            device_id={"patch": lax.rem(me + 2 * step + patches, patches)}, device_id_type=MESH,
        )

    def edge_copy(which, step):
        return pltpu.make_async_remote_copy(
            src_ref=edge_src, dst_ref=edges.at[which], send_sem=edge_send.at[which],
            recv_sem=edge_recv.at[which],
            device_id={"patch": lax.rem(partner + 2 * step + patches, patches)}, device_id_type=MESH,
        )

    mark("stats0")
    cp_feat.wait()
    x = feat[...].reshape(rows, channels).astype(F32)
    local_stats(0, x)
    mark("edges")
    cp_sconv.wait()
    whole_conv = sconv[...].astype(F32)
    edge_src[...] = jnp.where(core == 0, whole_conv[:, cols - 1], whole_conv[:, 0])
    pltpu.make_async_copy(vecs, vecs, v_sem).wait()
    vec = [vecs[pl.ds(t * channels, channels)].reshape(1, channels) for t in range(6)]
    cp_snorm.wait()

    def near(distance, visit):
        @pl.when(zo + distance < outer)
        def _():
            visit(zo + distance, 0)

        @pl.when(zo - distance >= 0)
        def _():
            visit(zo - distance, 1)

    def send_to(z):
        for b in range(images):
            x_copy(b, zo, yi, index(z, yi, core), xz_send).start()

    def send_far(first, last):
        def body(step, carry):
            near(last - step, lambda z, way: send_known(z))
            return carry

        def send_known(z):
            @pl.when(((zo >= hub) | (z < zo + 2)) & ((zo != 1) | (z != 0)))
            def _():
                send_to(z)

        lax.fori_loop(0, last - first + 1, body, 0)

    mark("barrier")
    pl.semaphore_wait(barrier, expected)
    mark("sends")

    def tell(z, carry):
        pl.semaphore_signal(
            ready, inc=1, device_id={"patch": index(z, yi, core)}, device_id_type=MESH
        )
        return carry

    @pl.when(zo == hub)
    def _():
        lax.fori_loop(0, hub, tell, 0)

    send_stats(0, lambda z: (zo >= hub) | (z <= zo))
    edge_copy(1, 0).start()

    @pl.when(yi == 0)
    def _():
        edge_copy(0, 1).start()
        halo_copy(0, 1).start()

    @pl.when(yi == 1)
    def _():
        edge_copy(2, -1).start()
        halo_copy(1, -1).start()

    for b in range(images):
        x_copy(b, zo, yi, index(zo, other, core), xy_send).start()
    if outer > 3:
        send_far(3, outer - 1)

    @pl.when(zo == 1)
    def _():
        send_to(0)

    @pl.when((yi == 0) & jnp.logical_not(row_first))
    def _():
        edge_copy(2, -1).start()
        halo_copy(1, -1).start()

    send_far(1, min(2, outer - 1))
    mark("ready")

    def late(step, carry):
        send_to(outer - 1 - step)
        return carry

    @pl.when(early)
    def _():
        pl.semaphore_wait(ready, 1)
        send_stats(0, lambda z: z > zo)

        @pl.when(yi == 1)
        def _():
            edge_copy(0, 1).start()
            halo_copy(0, 1).start()

        @pl.when((zo > 0) | (yi == 0))
        def _():
            lax.fori_loop(0, outer - 2 - zo, late, 0)

    def wait_x(b, z, y):
        x_copy(b, z, y, partner, xy_send).wait_recv()

    around = outer - 3
    sends_around = (zo == around) & (yi == 0)
    saved = (zo == outer - 1) & (yi == 1) & (around >= 0)

    def pass_y(z):
        for b in range(images):
            wait_x(b, z, yi)

            @pl.when(jnp.logical_not(saved & (z == around)))
            def _():
                x_copy(b, z, yi, index(zo, other, core), xy_send).start()

    def distance_at(step):
        return jnp.where(zo < outer // 2, outer - step, step)

    def each_far(visit):
        def body(step, carry):
            def one(z, way):
                @pl.when(z != first)
                def _():
                    visit(z)
            near(distance_at(step), one)
            return carry
        return body

    def stale_kv(z, sides=(0, 1)):
        places = [(b, at_slot(index(z, y, core))) for b in range(images) for y in sides]
        block = jnp.concatenate([xall[b, at, :] for b, at in places], axis=0)
        for w in range(2):
            made = dot(block, ws[w]).astype(BF16)
            for t, (b, at) in enumerate(places):
                kv[w, b, at, :] = made[t * cols:(t + 1) * cols]

    def push_kv(z, sides=(0, 1)):
        for y in sides:
            at = at_slot(index(z, y, core))
            ref = kv.at[:, :, at, :]

            @pl.when((z == zo) & (yi == y))
            def _():
                kv_copy(ref, 0).start()

            @pl.when((z != zo) | (yi != y))
            def _():
                kv_copy(ref, 1).start()

    def row_taps(i, first=False):
        for j in range(3):
            made = dot(lhs[i], wc[i, j])
            taps[j] = made if first else taps[j] + made

    def fill_row(i, cells):
        for b in range(images):
            lhs[i, b * cols:(b + 1) * cols, :] = cells[b]
        filler = jnp.zeros((lhs.shape[1] - rows - images, channels), F32)
        lhs[i, rows:, :] = jnp.concatenate([edges[i], filler], axis=0).astype(BF16)

    mark("pass0")
    pass_y(first)

    @pl.when((zo == 0) & (yi == 1))
    def _():
        lax.fori_loop(0, outer - 2, late, 0)

    mark("text")
    all_text.wait()
    for b in range(images):
        tk[b] = t_in[0, :, b, :]
        tv[b] = t_in[1, :, b, :]

    def outside(beside):
        mark("halo%d" % beside)
        below = (yi == 0) if beside else (yi == 1)
        which = jnp.where(below, 1, 0)
        row = 2 * which

        @pl.when(below & jnp.logical_not(row_last))
        def _():
            halo_copy(1, -1).wait_recv()
            edge_copy(2, -1).wait_recv()

        @pl.when(jnp.logical_not(below) & jnp.logical_not(row_first))
        def _():
            halo_copy(0, 1).wait_recv()
            edge_copy(0, 1).wait_recv()

        mark("conv%d" % beside)
        fill_row(row, halo[which])
        row_taps(row, beside)

    cp_wc.wait()
    outside(True)

    @pl.when(sends_around)
    def _():
        for b in range(images):
            wait_x(b, zo, other)
            x_copy(b, zo, other, index(outer - 1, yi, core), around_send).start()

    pass_far = each_far(pass_y)
    mark("wait0")
    table = finish_stats(0)
    mark("norm0")
    edge_copy(1, 0).wait_recv()
    centre = []
    for b in range(images):
        v = normed(x, table, b, vec[0], vec[1])
        centre.append((v * (1.0 / (1.0 + jnp.exp(-v)))).astype(BF16))
    fill_row(1, centre)
    mark("conv1")
    row_taps(1)
    mark("pass1b")
    done = jnp.where((zo == outer - 2) & (yi == 0), outer, 2)
    done = jnp.where((zo < outer // 2) | (yi == 0) & (zo == outer - 2), done, 1)
    lax.fori_loop(1, done, pass_far, 0)
    outside(False)
    mark("shift")
    place = lax.broadcasted_iota(jnp.int32, (cols, channels), 0)
    parts = []
    for b in range(images):
        at = slice(b * cols, (b + 1) * cols)
        left = pltpu.roll(taps[0, at], 1, 0)
        right = pltpu.roll(taps[2, at], cols - 1, 0)
        left_edge = jnp.where(core == 1, taps[0, rows + b:rows + b + 1], 0.0)
        right_edge = jnp.where(core == 0, taps[2, rows + b:rows + b + 1], 0.0)
        left = jnp.where(place == 0, left_edge, left)
        right = jnp.where(place == cols - 1, right_edge, right)
        conv = left + taps[1, at] + right
        parts.append(x[at] + conv + vec[2])
    hidden = jnp.concatenate(parts, axis=0)
    mark("stats1")
    local_stats(1, hidden)
    mark("send1")
    send_stats(1)
    mark("kv_own")
    wait_weights(0)

    @pl.when(jnp.logical_not(sends_around))
    def _():
        for b in range(images):
            wait_x(b, zo, other)

    stale_kv(zo)
    push_kv(zo)
    mark("pass2")
    lax.fori_loop(done, outer, pass_far, 0)

    def layer_kv(z):
        for b in range(images):
            wait_x(b, z, other)
        stale_kv(z)
        push_kv(z)

    mark("kv_first")
    layer_kv(first)

    def near_half(z):
        stale_kv(z, (yi,))
        push_kv(z, (yi,))

    def far_half(z):
        for b in range(images):
            wait_x(b, z, other)
        stale_kv(z, (other,))
        push_kv(z, (other,))

    mark("kv_far")
    lax.fori_loop(1, outer, each_far(near_half), 0)
    lax.fori_loop(1, outer, each_far(far_half), 0)
    mark("kvwait")
    own = at_slot(me)
    kv_copy(kv.at[:, :, own, :], 0).wait_send()
    kv_copy(kv.at[0], 1).wait_recv()
    wait_weights(1)
    mark("wait1")
    table = finish_stats(1)
    mark("norm1")
    attn_in = jnp.concatenate(
        [normed(hidden, table, b, vec[3], vec[4]) for b in range(images)], axis=0
    ).astype(BF16)
    for w in range(2):
        fresh = dot(attn_in, ws[w]).astype(BF16)
        for b in range(images):
            kv[w, b, own, :] = fresh[b * cols:(b + 1) * cols]
    mark("q")
    scale = HEAD_DIM ** -0.5
    lane = lax.broadcasted_iota(jnp.int32, (cols, LANES), 1)
    pairs = channels // LANES

    def heads(q, keys, values, together):
        for first in range(0, images, together):
            places = [
                (b, slice(p * LANES, (p + 1) * LANES))
                for b in range(first, first + together) for p in range(pairs)
            ]
            units = [
                (q[b * cols:(b + 1) * cols, at], keys[b, :, at], values[b, :, at])
                for b, at in places
            ]
            for (b, at), part in zip(places, attention_stages(units, lane)):
                att[b * cols:(b + 1) * cols, at] = part.astype(BF16)

    query = dot(attn_in, ws[2]).astype(BF16).astype(F32) * scale
    mark("attend")
    heads(query, kv.at[0], kv.at[1], images)
    mark("out_ln")
    mixed = hidden + dot(att[...], ws[3])
    centred = mixed - jnp.mean(mixed, axis=-1, keepdims=True)
    variance = jnp.mean(centred * centred, axis=-1, keepdims=True)
    layer_in = (centred * lax.rsqrt(variance + EPSILON) * vec[5]).astype(BF16)
    mark("cross")
    heads(dot(layer_in, ws[4]).astype(BF16).astype(F32) * scale, tk, tv, images)
    mark("out")
    out_ref[...] = mixed + dot(att[...], ws[5])

    mark("drain")
    all_stats(0).wait_send()
    all_stats(1).wait_send()
    def sent(blocks, send):
        for b in range(images):
            ref = xall.at[b, pl.ds(0, blocks * cols), :]
            pltpu.make_async_remote_copy(
                src_ref=ref, dst_ref=ref, send_sem=send, recv_sem=x_recv.at[0, 0],
                device_id={"patch": partner}, device_id_type=MESH,
            ).wait_send()

    sent(outer - 1, xz_send)


    @pl.when(saved)
    def _():
        sent(outer - 1, xy_send)

    @pl.when(jnp.logical_not(saved))
    def _():
        sent(outer, xy_send)

    @pl.when(sends_around)
    def _():
        sent(1, around_send)

    kv_copy(kv.at[0, :, pl.ds(0, (patches - 2) * cols)], 1).wait_send()
    edge_copy(1, 0).wait_send()

    @pl.when(jnp.logical_not(row_last))
    def _():
        halo_copy(0, 1).wait_send()
        edge_copy(0, 1).wait_send()

    @pl.when(jnp.logical_not(row_first))
    def _():
        halo_copy(1, -1).wait_send()
        edge_copy(2, -1).wait_send()


def solution(mesh):
    patches = mesh.shape["patch"]

    def on_device(
        features, stale_conv_in, stale_normed, first_gain, first_bias, conv_weight, conv_bias,
        second_gain, second_bias, query_weight, key_weight, value_weight, output_weight,
        layer_gain, cross_query, cross_output, text_keys, text_values,
    ):
        images, _, cols, channels = features.shape
        rows = images * cols
        span = patches * cols
        outer = patches // 4
        ctx = text_keys.shape[1]

        def flat(a):
            return a.reshape(images, cols, channels)

        dma = pltpu.SemaphoreType.DMA
        out = pl.pallas_call(
            functools.partial(kernel, patches, images, cols),
            out_shape=pltpu.VMEM((rows, channels), F32),
            in_specs=[pl.BlockSpec(memory_space=pltpu.HBM)] * 18,
            out_specs=pl.BlockSpec(memory_space=pltpu.VMEM),
            scratch_shapes=[
                pltpu.VMEM((images, cols, channels), BF16),
                pltpu.VMEM((images, cols, channels), BF16),
                pltpu.VMEM((images, span, channels), BF16),
                pltpu.VMEM((2, images, span, channels), BF16),
                pltpu.VMEM(conv_weight.shape, BF16),
                pltpu.VMEM((6, channels, channels), BF16),
                pltpu.VMEM((6 * channels,), F32),
                pltpu.VMEM((2, ctx, images, channels), BF16),
                pltpu.VMEM((images, ctx, channels), BF16),
                pltpu.VMEM((images, ctx, channels), BF16),
                pltpu.VMEM((2, patches, 2 * images, LANES), F32),
                pltpu.VMEM((2, images, cols, channels), BF16),
                pltpu.VMEM((images, channels), F32),
                pltpu.VMEM((3, images, channels), F32),
                pltpu.VMEM((3, rows + 16, channels), BF16),
                pltpu.VMEM((3, rows + 16, channels), F32),
                pltpu.VMEM((rows, channels), BF16),
                dma((2,)), dma((2,)), dma, dma, dma,
                dma((images, 2 * outer)), dma((2,)), dma,
                dma((2,)), dma((2,)), dma((3,)), dma((3,)), pltpu.SemaphoreType.REGULAR,
                dma((4,)), dma, dma((2,)), dma,
            ],
            compiler_params=pltpu.CompilerParams(
                collective_id=0, has_side_effects=True, vmem_limit_bytes=60000 * 1024
            ),
        )(
            flat(features), flat(stale_conv_in), flat(stale_normed), first_gain, first_bias,
            conv_weight, conv_bias, second_gain, second_bias, query_weight, key_weight,
            value_weight, output_weight, layer_gain, cross_query, cross_output,
            text_keys.transpose(1, 0, 2), text_values.transpose(1, 0, 2),
        )
        return out.reshape(features.shape)

    act = P("grp", "patch", None, None)
    text = P("grp", None, None)
    return jax.shard_map(
        on_device, mesh=mesh,
        in_specs=(act,) * 3 + (P(),) * 13 + (text,) * 2,
        out_specs=act, check_vma=False,
    )
```
